32 devices in a mesh: row: 8 (over z, x), col: 4 (over y, core).
Axes of the slice: x: 2, y: 2, z: 4, core: 2. Of those that a mesh axis runs over, the one named last changes fastest.
Arguments:
- tiles: bfloat16 [8, 4, 3, 256, 256], P('row', 'col'), as said below
- stack_index: int32 [8, 4, 3], P('row', 'col'), may hold values from 0 to 127, as said below
- block_mask: int32 [64, 64], replicated, may hold values from 0 to 1, as said below
Outputs:
- purified: bfloat16 [8, 4, 3, 256, 256], P('row', 'col')
The draws below stay inside these ranges and needn't reach their ends.
Inputs may be any that keep to these rules, and one draw needn't show every extreme that they name: `block_mask`: the region of one device (8 x 16 blocks) holds at most 3 occupied blocks; some region holds exactly 3 in every draw. `stack_index`: block (a, b) of a device's region is numbered a * 16 + b. A device's 3 entries are distinct and include every occupied block of its region; a slot naming an unoccupied block holds a tile that P does not use. `tiles`: A slot's tile is P's block named by stack_index when that block is occupied.
All inputs are finite; a program needn't handle non-finite values.
Results may differ from the reference program's by a relative error of at most 0.0051.
Values may be sent and summed in bfloat16 or wider, within the bound.
A program may use at most 64 MiB of HBM per device.

```python
import jax
import jax.numpy as jnp
from jax import lax

NB = 64
BS = 256
SLOTS = 3
BR = 8
BC = 16
N_ROW = 8
N_COL = 4


def to_regions(table):
    return table.reshape(N_ROW, BR, N_COL, BC).transpose(0, 2, 1, 3).reshape(N_ROW, N_COL, BR * BC)


def block_layout(key):
    cluster_key = jax.random.fold_in(key, 301)
    anchor_row_key = jax.random.fold_in(key, 302)
    anchor_col_key = jax.random.fold_in(key, 303)
    noise_key = jax.random.fold_in(key, 304)
    mixing_key = jax.random.fold_in(key, 305)
    cluster = jax.random.randint(cluster_key, (NB,), 0, max(NB // 8, 1), dtype=jnp.int32)
    row_iota = jnp.arange(NB, dtype=jnp.int32)[:, None]
    col_iota = jnp.arange(NB, dtype=jnp.int32)[None, :]
    anchor_row = jax.random.randint(anchor_row_key, (), 0, N_ROW, dtype=jnp.int32)
    anchor_col = jax.random.randint(anchor_col_key, (), 0, N_COL, dtype=jnp.int32)
    favoured = (row_iota // BR == anchor_row) & (col_iota // BC == anchor_col)
    candidate = ((cluster[:, None] == cluster[None, :]) | favoured).astype(jnp.int32)
    noise_draw = jax.random.randint(noise_key, (NB, NB), 0, 1024, dtype=jnp.int32)
    priority = candidate * 4096 + noise_draw
    local_count = BR * BC
    local_iota = jnp.arange(local_count, dtype=jnp.int32)
    region_priority = to_regions(priority) * local_count + local_iota
    _, picked = lax.top_k(region_priority, SLOTS)
    picked = picked.astype(jnp.int32)
    kept_slot = jnp.sum((picked[:, :, :, None] == local_iota[None, None, None, :]).astype(jnp.int32), axis=2)
    region_mask = to_regions(candidate) * kept_slot
    occupied = region_mask.reshape(N_ROW, N_COL, BR, BC).transpose(0, 2, 1, 3).reshape(NB, NB)
    mixing = jax.random.randint(mixing_key, (N_ROW, N_COL, SLOTS), 0, 4096, dtype=jnp.int32) * SLOTS + jnp.arange(SLOTS, dtype=jnp.int32)
    placement = jnp.argsort(mixing, axis=2)
    stack_ids = jnp.take_along_axis(picked, placement, axis=2)
    return (occupied, stack_ids)


def draw_block_mask(key, part):
    return block_layout(key)[0]


def draw_stack_index(key, part):
    return block_layout(key)[1]


def draw_tiles(key, part):
    occupied, stack_ids = block_layout(key)
    noise_key = jax.random.fold_in(key, 201)
    tile_shape = (N_ROW, N_COL, SLOTS, BS, BS)
    spread = 1.0 / BS ** 0.5
    noise_draw = spread * jax.random.normal(noise_key, tile_shape, jnp.float32)
    band_row = jnp.arange(N_ROW, dtype=jnp.int32)[:, None, None]
    band_col = jnp.arange(N_COL, dtype=jnp.int32)[None, :, None]
    on_diagonal = band_row * BR + stack_ids // BC == band_col * BC + stack_ids % BC
    identity = jnp.eye(BS, dtype=jnp.float32)
    values = noise_draw + 0.5 * on_diagonal.astype(jnp.float32)[:, :, :, None, None] * identity
    return values.astype(jnp.bfloat16)


def setup_inputs(seed: int = 0) -> dict:
    key_of = jax.random.split(jax.random.key(seed), 4)
    return {
        "tiles": draw_tiles(jax.random.fold_in(key_of[3], 71), 0),
        "stack_index": draw_stack_index(jax.random.fold_in(key_of[3], 71), 0),
        "block_mask": draw_block_mask(jax.random.fold_in(key_of[3], 71), 0),
    }


def reference(tiles, stack_index, block_mask):
    total_slots = N_ROW * N_COL * SLOTS
    flat_tiles = tiles.reshape(total_slots, BS, BS)
    places = jnp.arange(total_slots, dtype=jnp.int32)
    device_id = places // SLOTS
    device_row = device_id // N_COL
    device_col = device_id % N_COL
    flat_ids = stack_index.reshape(total_slots).astype(jnp.int32)
    global_row = (device_row * BR + flat_ids // BC).astype(jnp.int32)
    global_col = (device_col * BC + flat_ids % BC).astype(jnp.int32)
    valid = block_mask[global_row, global_col] > 0
    slot_of = jnp.zeros((NB, NB), jnp.int32).at[global_row, global_col].set(places)

    def product(left_flat, right_flat):
        def per_slot(columns):
            block_row, block_col, live = columns

            def compute(unused):
                def inner(inner_block, total):
                    weight = block_mask[block_row, inner_block] * block_mask[inner_block, block_col]

                    def add_term(running):
                        left_tile = left_flat[slot_of[block_row, inner_block]]
                        right_tile = right_flat[slot_of[inner_block, block_col]]
                        return running + jnp.dot(left_tile, right_tile, preferred_element_type=jnp.float32)

                    def keep_term(running):
                        return running

                    return lax.cond(weight > 0, add_term, keep_term, total)

                return lax.fori_loop(0, NB, inner, jnp.zeros((BS, BS), jnp.float32))

            def skipped(unused):
                return jnp.zeros((BS, BS), jnp.float32)

            return lax.cond(live, compute, skipped, 0)

        return lax.map(per_slot, (global_row, global_col, valid))

    square = product(flat_tiles, flat_tiles).astype(jnp.bfloat16)
    cube_sum = product(square, flat_tiles)
    valid_float = valid.astype(jnp.float32)
    purified = (3.0 * square.astype(jnp.float32) - 2.0 * cube_sum) * valid_float[:, None, None]
    return purified.astype(jnp.bfloat16).reshape(N_ROW, N_COL, SLOTS, BS, BS)
```

```python
import functools

import jax
import jax.numpy as jnp
from jax import lax
from jax.experimental import pallas as pl
from jax.experimental.pallas import tpu as pltpu
from jax.sharding import PartitionSpec as P

MESH = pl.DeviceIdType.MESH
VMEM = pl.BlockSpec(memory_space=pltpu.VMEM)
SMEM = pl.BlockSpec(memory_space=pltpu.SMEM)


def send(src, dst, send_sem, recv_sem, row, col):
    return pltpu.make_async_remote_copy(
        src_ref=src,
        dst_ref=dst,
        send_sem=send_sem,
        recv_sem=recv_sem,
        device_id=(row, col),
        device_id_type=MESH,
    )


def greet(row_size, col_size, row, col, with_rows):
    barrier = pltpu.get_barrier_semaphore()
    count = col_size - 1
    for step in range(1, col_size):
        peer = lax.rem(col + step, col_size)
        pl.semaphore_signal(barrier, inc=1, device_id=(row, peer), device_id_type=MESH)
    if with_rows:
        count += row_size - 1
        for step in range(1, row_size):
            peer = lax.rem(row + step, row_size)
            pl.semaphore_signal(barrier, inc=1, device_id=(peer, col), device_id_type=MESH)
    pl.semaphore_wait(barrier, count)


class ColGather:
    def __init__(self, row, col, col_size, slots, own, panel, sems):
        self.row, self.col, self.slots = row, col, slots
        self.own, self.panel, self.sems = own, panel, sems
        self.chips = col_size // 2
        self.chip, self.core = col // 2, lax.rem(col, 2)
        self.partner = col + 1 - 2 * self.core

    def across(self, step, slot):
        target = 2 * lax.rem(self.chip + step, self.chips) + self.core
        return send(
            self.own.at[slot], self.panel.at[self.col, slot],
            self.sems.at[0, step - 1, slot], self.sems.at[1, step - 1, slot], self.row, target,
        )

    def beside(self, step, slot):
        origin = 2 * lax.rem(self.chip + self.chips - step, self.chips) + self.core
        src = self.own.at[slot] if step == 0 else self.panel.at[origin, slot]
        return send(
            src, self.panel.at[origin, slot],
            self.sems.at[2, step, slot], self.sems.at[3, step, slot], self.row, self.partner,
        )

    def start(self):
        for slot in range(self.slots):
            for step in range(1, self.chips):
                self.across(step, slot).start()
        for slot in range(self.slots):
            self.beside(0, slot).start()

    def origin(self, step, core):
        return 2 * lax.rem(self.chip + self.chips - step, self.chips) + core

    def forward(self, use=None):
        for slot in range(self.slots):
            for step in range(1, self.chips):
                self.across(step, slot).wait_recv()
                self.beside(step, slot).start()
                if use is not None:
                    use(self.origin(step, self.core), slot)

    def collect(self, use, steps):
        for step in steps:
            for slot in range(self.slots):
                self.beside(step, slot).wait_recv()
                if use is not None:
                    use(self.origin(step, 1 - self.core), slot)

    def settle(self):
        for step in range(self.chips):
            for slot in range(self.slots):
                if step:
                    self.across(step, slot).wait_send()
                self.beside(step, slot).wait_send()


def dense_kernel(
    row_size, col_size, tiles, ids, mask, out, left, right, squares, square, total, left_ids, right_ids, ids_out,
    left_labels, right_labels, col_sems, square_sems, line_sems, side_sems, row_id_sems, col_id_sems, label_sems,
):
    row, col = lax.axis_index("row"), lax.axis_index("col")
    slots, side = tiles.shape[0], tiles.shape[1]
    half = side // 2
    length = row_size // 2
    place, lane = row // 2, lax.rem(row, 2)
    mate = row + 1 - 2 * lane

    lane_iota = lax.broadcasted_iota(jnp.int32, (8, 128), 1)
    packed = jnp.full((8, 128), -1, jnp.int32)
    for slot in range(slots):
        packed = jnp.where(lane_iota == slot, ids[0, slot], packed)
    ids_out[...] = packed
    greet(row_size, col_size, row, col, True)

    pieces = [(slot, 0, side, False) for slot in range(slots - 1)]
    cut = side * 64 // 256
    pieces += [(slots - 1, cut, side - cut, False)]
    early = (slots - 1, 0, cut, True)
    mine = [early] + pieces
    count = len(mine)

    def view(ref, piece, origin=None):
        slot, first, rows, _ = piece
        if origin is None:
            return ref.at[slot, pl.ds(first, rows)]
        return ref.at[origin, slot, pl.ds(first, rows)]

    def to_mate(index, at):
        piece = mine[index]
        origin = 2 * at + lane
        return send(
            view(right, piece, origin), view(right, piece, origin),
            side_sems.at[0, at, index], side_sems.at[1, at, index], mate, col,
        )

    def own_to_mate(index):
        piece = mine[index]
        return send(
            view(tiles, piece), view(right, piece, row),
            side_sems.at[0, place, index], side_sems.at[1, place, index], mate, col,
        )

    def from_mate(index, at):
        piece = mine[index]
        origin = 2 * at + 1 - lane
        return send(
            view(right, piece, origin), view(right, piece, origin),
            side_sems.at[0, at, index], side_sems.at[1, at, index], mate, col,
        )

    def along(way, step, index, first=False):
        heading = 1 if way == 0 else -1
        piece = mine[0] if index == count else mine[index]
        on_lane = 1 - lane if index == count else lane
        origin = 2 * (place - heading * step) + on_lane
        src = view(tiles, piece) if first and index < count else view(right, piece, origin)
        return send(
            src, view(right, piece, origin),
            line_sems.at[way, 0, step, index], line_sems.at[way, 1, step, index],
            row + 2 * heading, col,
        )

    def landing(way, step, index):
        heading = 1 if way == 0 else -1
        piece = mine[0] if index == count else mine[index]
        on_lane = 1 - lane if index == count else lane
        origin = 2 * (place - heading * (step + 1)) + on_lane
        return send(
            view(right, piece, origin), view(right, piece, origin),
            line_sems.at[way, 0, step, index], line_sems.at[way, 1, step, index],
            row + 2 * heading, col,
        )

    can_send = (place + 1 < length, place > 0)

    def arrives(way, step):
        return place - step >= 1 if way == 0 else place + step + 1 < length

    def goes(way, step):
        if way == 0:
            return (place - step >= 0) & (place + 1 < length)
        return (place + step < length) & (place > 0)

    def id_row(step):
        return send(
            ids_out, right_ids.at[row], row_id_sems.at[0, step], row_id_sems.at[1, step],
            lax.rem(row + step, row_size), col,
        )

    def id_col(step):
        return send(
            ids_out, left_ids.at[col], col_id_sems.at[0, step], col_id_sems.at[1, step],
            row, lax.rem(col + step, col_size),
        )

    for step in range(1, row_size):
        id_row(step).start()
    for step in range(1, col_size):
        id_col(step).start()

    left_gather = ColGather(row, col, col_size, slots, tiles, left, col_sems)
    left_gather.start()
    own_to_mate(0).start()
    for index in range(count):
        for way in range(2):
            @pl.when(can_send[way])
            def _():
                along(way, 0, index, True).start()
        if index:
            own_to_mate(index).start()


    from_mate(0, place).wait_recv()
    for way in range(2):
        @pl.when(can_send[way])
        def _():
            along(way, 0, count).start()

    right[row] = tiles[...]
    left[col] = tiles[...]
    right_ids[row] = packed
    left_ids[col] = packed

    def turn(step, unused):
        for index in list(range(count)) + [count]:
            for way in range(2):
                @pl.when(arrives(way, step))
                def _():
                    landing(way, step, index).wait_recv()

                    @pl.when(can_send[way])
                    def _():
                        along(way, step + 1, index).start()

                    if 0 < index < count:
                        heading = 1 if way == 0 else -1
                        to_mate(index, place - heading * (step + 1)).start()
        return unused

    block_rows, block_cols = mask.shape[0] // row_size, mask.shape[1] // col_size
    owns = []
    for slot in range(slots):
        own = ids[0, slot]
        own_row, own_col = own // block_cols, lax.rem(own, block_cols)
        out_row, out_col = row * block_rows + own_row, col * block_cols + own_col
        owns.append((own_row, own_col, out_row, out_col, mask[out_row, out_col] > 0))

    def find(labels, region, wanted):
        spot, found = jnp.int32(0), labels[region, 0, 0] == wanted
        for other in range(1, slots):
            same = labels[region, 0, other] == wanted
            spot = jnp.where(same, other, spot)
            found = found | same
        return spot, found

    def square_term(origin, place):
        label = right_labels[origin, 0, place]
        inner = origin * block_rows + label // block_cols
        band = inner // block_cols
        chosen = []
        for own_row, own_col, out_row, out_col, live in owns:
            spot, found = find(left_labels, band, own_row * block_cols + lax.rem(inner, block_cols))
            use = live & found & (lax.rem(label, block_cols) == own_col)
            use = use & (mask[out_row, inner] > 0) & (mask[inner, out_col] > 0)
            tile = left[band, spot]
            chosen.append(jnp.where(use, tile, jnp.zeros_like(tile)))
        term = jnp.dot(
            jnp.concatenate(chosen, axis=0), right[origin, place], preferred_element_type=jnp.float32
        )
        total[...] += term.reshape(total.shape)

    def cube_term(origin, place):
        label = left_labels[origin, 0, place]
        inner = origin * block_cols + lax.rem(label, block_cols)
        band = inner // block_rows
        piece = squares[origin, place]
        for slot, (own_row, own_col, out_row, out_col, live) in enumerate(owns):
            spot, found = find(right_labels, band, lax.rem(inner, block_rows) * block_cols + own_col)
            use = live & found & (label // block_cols == own_row)
            use = use & (mask[out_row, inner] > 0) & (mask[inner, out_col] > 0)
            tile = right[band, spot]
            total[slot] += jnp.dot(
                piece, jnp.where(use, tile, jnp.zeros_like(tile)), preferred_element_type=jnp.float32
            )

    def stack_terms(origin, wait=None):
        for slot in range(slots):
            if wait is not None:
                wait(slot)
            square_term(origin, slot)

    def mate_terms(at):
        stack_terms(2 * at + 1 - lane, lambda slot: from_mate(slot + 1, at).wait_recv())

    def consume(step):
        for way in range(2):
            @pl.when(arrives(way, step))
            def _():
                heading = 1 if way == 0 else -1
                stack_terms(2 * (place - heading * (step + 1)) + lane)
        for way in range(2):
            @pl.when(arrives(way, step))
            def _():
                heading = 1 if way == 0 else -1
                mate_terms(place - heading * (step + 1))

    total[...] = jnp.zeros_like(total)
    turn(0, 0)
    for step in range(1, row_size):
        id_row(step).wait()
    for step in range(1, col_size):
        id_col(step).wait()
    copies = (
        pltpu.make_async_copy(left_ids, left_labels, label_sems.at[0]),
        pltpu.make_async_copy(right_ids, right_labels, label_sems.at[1]),
    )
    for copy in copies:
        copy.start()
    for copy in copies:
        copy.wait()
    left_gather.forward()
    left_gather.collect(None, range(left_gather.chips))
    stack_terms(row)
    mate_terms(place)

    def advance(step, unused):
        turn(step, 0)
        consume(step - 1)
        return unused

    lax.fori_loop(1, length - 1, advance, 0)
    consume(length - 2)

    square[...] = total[...].astype(square.dtype)

    square_gather = ColGather(row, col, col_size, slots, square, squares, square_sems)

    def keep(slot, unused):
        squares[col, slot] = square[slot]
        for step in range(1, square_gather.chips):
            square_gather.across(step, slot).start()
        square_gather.beside(0, slot).start()
        return unused

    lax.fori_loop(0, slots, keep, 0)
    total[...] = jnp.zeros_like(total)
    for slot in range(slots):
        cube_term(col, slot)
    square_gather.collect(cube_term, [0])
    square_gather.forward(cube_term)
    square_gather.collect(cube_term, range(1, square_gather.chips))
    out[...] = (3.0 * square[...].astype(jnp.float32) - 2.0 * total[...]).astype(out.dtype)

    left_gather.settle()
    square_gather.settle()

    def settle(step, unused):
        for index in range(count + 1):
            for way in range(2):
                @pl.when(goes(way, step))
                def _():
                    along(way, step, index).wait_send()
        return unused

    lax.fori_loop(0, length - 1, settle, 0)
    own_to_mate(0).wait_send()

    def collect(at, unused):
        for index in range(1, count):
            to_mate(index, at).wait_send()
        return unused

    lax.fori_loop(0, length, collect, 0)

X_SLOTS = 3
Z_SLOTS = 4
TERMS = 4
PARTS = 4
F32, BF16 = jnp.float32, jnp.bfloat16


def iota(shape, axis):
    return lax.broadcasted_iota(jnp.int32, shape, axis)


def plan_kernel(row_size, col_size, slots, mask, out, tile_row, tile_col, tile_spot, reach, table, across, stops):
    blocks, lanes = mask.shape[0], 128
    block_rows, block_cols = blocks // row_size, blocks // col_size
    length = row_size // 2
    lines = 4 * col_size
    row, col = lax.axis_index("row"), lax.axis_index("col")
    place, lane = row // 2, lax.rem(row, 2)
    dot = functools.partial(jnp.dot, preferred_element_type=F32)

    occupied = mask[...].astype(F32)
    grid = occupied.astype(BF16)
    row_of, lane_of = iota((blocks, lanes), 0), iota((blocks, lanes), 1)
    spread = row_of - lax.rem(lane_of, block_cols)
    keep = lax.rem(row_of, block_rows) == lane_of // block_cols
    before = (iota((lanes, lanes), 0) <= iota((lanes, lanes), 1)).astype(F32).astype(BF16)
    region_of, spot_of = iota((row_size, lanes), 0), iota((row_size, lanes), 1)
    home = spot_of // slots
    tile_home = iota((1, lanes), 1) // slots
    spot_value = (spot_of + 1).astype(F32)
    at = row_of.astype(F32)

    def groups(value):
        return jnp.sum(value.reshape(row_size, block_rows, lanes), axis=1)

    for panel in range(col_size):
        pick = (spread == panel * block_cols).astype(F32).astype(BF16)
        flat = groups(jnp.where(keep, dot(grid, pick), 0.0))
        rank = dot(flat.astype(BF16), before)
        spots = jnp.zeros((row_size, lanes), F32)
        for slot in range(slots):
            found = jnp.where((rank == slot + 1) & (flat > 0), spot_value, 0.0)
            found = jnp.sum(found, axis=1, keepdims=True)
            spots = jnp.where(spot_of == region_of * slots + slot, found, spots)
        spot = jnp.sum(spots, axis=0, keepdims=True) - 1.0
        high = jnp.floor((spot + 0.5) / block_cols)
        block_row = jnp.where(spot >= 0, tile_home.astype(F32) * block_rows + high, -1.0)
        block_col = jnp.where(spot >= 0, panel * block_cols + spot - high * block_cols, -1.0)
        tile_spot[pl.ds(panel, 1), :] = spot
        tile_row[pl.ds(panel, 1), :] = block_row
        tile_col[pl.ds(panel, 1), :] = block_col
        by_row = dot(grid, (at == block_row).astype(F32).astype(BF16))
        by_col = dot(grid, (at == block_col).astype(F32).astype(BF16))
        wanted = (groups(by_row * by_col) > 0) & (region_of != home)
        for side in range(2):
            for way in range(2):
                step = region_of // 2 + 1 if way == 0 else length - region_of // 2
                far = jnp.where(wanted & (lax.rem(region_of, 2) == side), step.astype(F32), 0.0)
                reach[pl.ds((side * 2 + way) * col_size + panel, 1), :] = jnp.max(far, axis=0, keepdims=True)

    far = reach[...]
    line, tile = iota((lines, lanes), 0), iota((lines, lanes), 1)
    side, way = line // (2 * col_size), lax.rem(line // col_size, 2)
    origin, number = tile // slots, lax.rem(tile, slots)
    begin = jnp.where(way == 0, origin // 2, length - 1 - origin // 2)
    begin = jnp.minimum(begin, jnp.where(tile < row_size * slots, begin, length))
    straight = lax.rem(origin, 2) == side
    crosses = jnp.where((far > 0) & jnp.logical_not(straight), 1.0, 0.0)
    order = jnp.zeros((lines, lanes), F32)
    for back in range(1, slots):
        order += jnp.where(number >= back, pltpu.roll(crosses, back, 1), 0.0)
    across[...] = jnp.where(crosses > 0, order + 1.0, 0.0)
    trouble = jnp.where((crosses > 0) & (order >= X_SLOTS - 1), 1.0, 0.0)
    rank_value = (128 * tile).astype(F32)
    table_now = jnp.zeros((lines, lanes), F32)
    stop = jnp.zeros((lines, lanes), F32)
    number_value = number.astype(F32)
    for step in range(length - 1):
        fresh = begin == step
        ready = jnp.where(fresh, jnp.where(straight, 0.0, order + 1.0), stop)
        code = jnp.where(
            fresh, jnp.where(straight, number_value, slots + order), slots + X_SLOTS + stop
        )
        left = jnp.where((far > step + 1) & (begin <= step), 1.0, 0.0)
        key = far * (128 * 128) - rank_value + code + 1.0
        for turn in range(Z_SLOTS):
            live = jnp.where((left > 0) & (ready <= turn), key, 0.0)
            best = jnp.max(live, axis=1, keepdims=True)
            taken = (live == best) & (live > 0)
            stop = jnp.where(taken, float(turn), stop)
            left = jnp.where(taken, 0.0, left)
            table_now = jnp.where(tile == step * 8 + turn, best, table_now)
            if turn == Z_SLOTS - 2:
                trouble = jnp.maximum(trouble, left)
        trouble = jnp.maximum(trouble, 2.0 * left)
        stops[step] = stop
    table_now = table_now - 128 * jnp.floor(table_now / 128)
    table[...] = jnp.maximum(table_now - 1.0, 0.0)

    here, there = (lane * 2) * col_size + col, (lane * 2 + 1) * col_size + col
    other = (1 - lane) * 2 * col_size + col
    tile, tile_number = iota((1, lanes), 1), lax.rem(iota((1, lanes), 1), slots)
    tile_place = tile_home // 2
    my_rows, my_cols = tile_row[pl.ds(col, 1), :], tile_col[pl.ds(col, 1), :]
    beyond = stops[jnp.maximum(place - 1, 0), pl.ds(here, 1), :]
    under = stops[jnp.maximum(length - 2 - place, 0), pl.ds(there, 1), :]
    spot = jnp.where(tile_place < place, slots + X_SLOTS + beyond, slots + X_SLOTS + Z_SLOTS + under)
    spot = jnp.where(tile_place == place, slots - 1 + across[pl.ds(here, 1), :], spot)
    spot = jnp.where(tile_home == row, tile_number.astype(F32), spot)

    inside = iota((blocks, blocks), 0), iota((blocks, blocks), 1)
    same_rows = inside[0] // block_rows == inside[1] // block_rows
    same_cols = inside[0] // block_cols == inside[1] // block_cols
    lower = (same_rows & (inside[1] < inside[0])).astype(F32).astype(BF16)
    whole = same_cols.astype(F32).astype(BF16)
    upper = (same_cols & (inside[0] < inside[1])).astype(F32).astype(BF16)
    ranks = dot(dot(lower, grid).astype(BF16), whole) + dot(grid, upper)
    labels = ranks + ((inside[1] // block_cols) * slots).astype(F32)
    fan = jnp.max(jnp.max(dot(grid, grid) * occupied, axis=1, keepdims=True), axis=0, keepdims=True)

    chosen = (at == my_rows).astype(F32).astype(BF16)
    met, named = dot(grid, chosen), dot(labels.astype(BF16), chosen)
    sub = iota((8, lanes), 0)
    pairs = jnp.zeros((8, lanes), F32)
    for slot in range(slots):
        mine = tile == row * slots + slot
        out_row = jnp.sum(jnp.where(mine, my_rows, 0.0), axis=1, keepdims=True)
        out_col = jnp.sum(jnp.where(mine, my_cols, 0.0), axis=1, keepdims=True)
        on_row = at == out_row
        joins = jnp.sum(jnp.where(on_row, met, 0.0), axis=0, keepdims=True)
        name = jnp.sum(jnp.where(on_row, named, 0.0), axis=0, keepdims=True)
        use = (joins > 0) & (my_cols == out_col) & (my_rows >= 0)
        pairs = jnp.where((sub == slot) & use, name * 64 + spot + 1, pairs)
    product = jnp.zeros((8, lanes), F32)
    column = iota((8, lanes), 1)
    for term in range(TERMS):
        best = jnp.max(pairs, axis=1, keepdims=True)
        pairs = jnp.where(pairs == best, 0.0, pairs)
        product = jnp.where(column == term, best, product)

    level = jnp.max(jnp.max(trouble, axis=1, keepdims=True), axis=0, keepdims=True)
    level = jnp.where(fan > TERMS, 2.0, level)
    result = jnp.where(sub == 0, table[pl.ds(here, 1), :], 0.0)
    result = jnp.where(sub == 1, table[pl.ds(there, 1), :], result)
    result = jnp.where(sub == 2, across[pl.ds(other, 1), :], result)
    for slot in range(slots):
        result = jnp.where(sub == 3 + slot, jnp.sum(jnp.where(sub == slot, product, 0.0), axis=0, keepdims=True), result)
    result = jnp.where(sub == 6, tile_spot[pl.ds(col, 1), :], result)
    result = jnp.where(sub == 7, level, result)
    out[...] = result.astype(jnp.int32)


def make_plan(mesh, mask, slots):
    row_size, col_size = mesh.shape["row"], mesh.shape["col"]
    panel = pltpu.VMEM((col_size, 128), F32)
    lines = (4 * col_size, 128)
    return pl.pallas_call(
        functools.partial(plan_kernel, row_size, col_size, slots),
        out_shape=jax.ShapeDtypeStruct((8, 128), jnp.int32),
        in_specs=[VMEM],
        out_specs=VMEM,
        scratch_shapes=[panel, panel, panel] + [pltpu.VMEM(lines, F32)] * 3
        + [pltpu.VMEM((row_size // 2 - 1, *lines), F32)],
        name="plan",
    )(mask)


def sparse_kernel(
    row_size, col_size, x_slots, z_slots, lag, plan, tiles, ids, out, canon, left, held, squares, square, final,
    x_out, z_out, col_sems, square_sems, x_sems, z_sems,
):
    row, col = lax.axis_index("row"), lax.axis_index("col")
    slots, side = tiles.shape[0], tiles.shape[1]
    rows = side // PARTS
    length = row_size // 2
    place, lane = row // 2, lax.rem(row, 2)
    mate = row + 1 - 2 * lane
    chips = col_size // 2
    chip, core = col // 2, lax.rem(col, 2)

    barrier = pltpu.get_barrier_semaphore()

    def hello(to_row, to_col):
        pl.semaphore_signal(barrier, inc=1, device_id=(to_row, to_col), device_id_type=MESH)

    hello(mate, col)
    hello(row, col + 1 - 2 * core)
    for step in range(1, chips):
        hello(row, 2 * lax.rem(chip + step, chips) + core)
    for way in range(2):
        @pl.when((place + 1 < length) if way == 0 else (place > 0))
        def _():
            hello(row + 2 - 4 * way, col)

    for number in range(slots):
        name = plan[6, row * slots + number]
        tile = jnp.zeros((side, side), tiles.dtype)
        for slot in range(slots):
            tile = jnp.where((ids[0, slot] == name) & (name >= 0), tiles[slot], tile)
        canon[number] = tile
    for slot in range(x_slots):
        tile = canon[0]
        for number in range(1, slots):
            tile = jnp.where(plan[2, row * slots + number] == slot + 1, canon[number], tile)
        x_out[slot] = tile

    ends = jnp.where(place == 0, 1, 0) + jnp.where(place + 1 == length, 1, 0)
    pl.semaphore_wait(barrier, 2 + chips - 1 + 2 - ends)

    def x_copy(slot, part):
        span = pl.ds(part * rows, rows)
        return send(
            x_out.at[slot, span], held.at[slots + slot, span],
            x_sems.at[0, slot, part], x_sems.at[1, slot, part], mate, col,
        )

    def z_copy(way, slot, part):
        span = pl.ds(part * rows, rows)
        return send(
            z_out.at[way, slot, span], held.at[slots + X_SLOTS + way * Z_SLOTS + slot, span],
            z_sems.at[way, 0, slot, part], z_sems.at[way, 1, slot, part], row + 2 - 4 * way, col,
        )

    for slot in range(x_slots):
        for part in range(PARTS):
            x_copy(slot, part).start()
    left_gather = ColGather(row, col, col_size, slots, canon, left, col_sems)
    left_gather.start()

    steps = z_slots * PARTS
    lead = jnp.where(2 * place < length, 0, 1)
    hops = jnp.where(lead == 0, place, length - 1 - place)
    shift = (length - 1 - 2 * hops) * lag

    def hop(way, step, first):
        slot, part = step // PARTS, lax.rem(step, PARTS)
        done = jnp.where(way == 0, place, length - 1 - place)

        @pl.when(done + 1 < length)
        def _():
            @pl.when(done > 0)
            def _():
                z_copy(way, slot, part).wait_recv()

            if first:
                @pl.when((slot >= 1) & (slot <= x_slots))
                def _():
                    x_copy(slot - 1, part).wait_recv()

            span = pl.ds(part * rows, rows)
            code = plan[way, done * 8 + slot]
            piece = canon[0, span]
            for number in range(1, slots):
                piece = jnp.where(code == number, canon[number, span], piece)
            z_out[way, slot, span] = piece
            for other in range(x_slots):
                @pl.when(other < slot)
                def _():
                    z_out[way, slot, span] = jnp.where(
                        code == slots + other, held[slots + other, span], z_out[way, slot, span]
                    )

            for other in range(z_slots):
                @pl.when((other <= slot) & (done > 0))
                def _():
                    z_out[way, slot, span] = jnp.where(
                        code == slots + X_SLOTS + other,
                        held[slots + X_SLOTS + way * Z_SLOTS + other, span], z_out[way, slot, span],
                    )

            z_copy(way, slot, part).start()

    def advance(step, unused):
        @pl.when(step < steps)
        def _():
            hop(lead, step, True)

        @pl.when((step >= shift) & (step < steps + shift))
        def _():
            hop(1 - lead, step - shift, False)

        return unused

    lax.fori_loop(0, steps + (length - 1) * lag, advance, 0)
    left_gather.forward()

    for number in range(slots):
        held[number] = canon[number]
        left[col, number] = canon[number]

    def arrive(step, unused):
        slot, part = step // PARTS, lax.rem(step, PARTS)
        for way in range(2):
            @pl.when((place + 1 == length) if way == 0 else (place == 0))
            def _():
                z_copy(way, slot, part).wait_recv()
        return unused

    lax.fori_loop(0, steps, arrive, 0)
    left_gather.collect(None, range(left_gather.chips))

    def sum_terms(panel, number):
        total = jnp.zeros((side, side), F32)
        for term in range(TERMS):
            code = plan[3 + number, term]
            pair = jnp.maximum(code - 1, 0)
            name, spot = pair // 64, lax.rem(pair, 64)
            tile = panel[name // slots, lax.rem(name, slots)]
            total += jnp.dot(
                jnp.where(code > 0, tile, jnp.zeros_like(tile)), held[spot], preferred_element_type=F32
            )
        return total

    square_gather = ColGather(row, col, col_size, slots, square, squares, square_sems)

    def first(number, unused):
        tile = sum_terms(left, number).astype(square.dtype)
        square[number] = tile
        squares[col, number] = tile
        for step in range(1, chips):
            square_gather.across(step, number).start()
        square_gather.beside(0, number).start()
        return unused

    lax.fori_loop(0, slots, first, 0)
    square_gather.forward()
    square_gather.collect(None, range(chips))

    def second(number, unused):
        final[number] = (3.0 * square[number].astype(F32) - 2.0 * sum_terms(squares, number)).astype(final.dtype)
        return unused

    lax.fori_loop(0, slots, second, 0)
    for slot in range(slots):
        tile = jnp.zeros((side, side), out.dtype)
        for number in range(slots):
            name = plan[6, row * slots + number]
            tile = jnp.where((ids[0, slot] == name) & (name >= 0), final[number], tile)
        out[slot] = tile

    left_gather.settle()
    square_gather.settle()

    def settle_x(step, unused):
        x_copy(step // PARTS, lax.rem(step, PARTS)).wait_send()
        return unused

    lax.fori_loop(0, x_slots * PARTS, settle_x, 0)

    def settle_z(step, unused):
        slot, part = step // PARTS, lax.rem(step, PARTS)
        for way in range(2):
            @pl.when((place + 1 < length) if way == 0 else (place > 0))
            def _():
                z_copy(way, slot, part).wait_send()
        return unused

    lax.fori_loop(0, steps, settle_z, 0)


def sparse_step(mesh, x_slots, z_slots, barrier_id, plan, stack, ids):
    row_size, col_size = mesh.shape["row"], mesh.shape["col"]
    chips = col_size // 2
    slots, side, _ = stack.shape
    dma = pltpu.SemaphoreType.DMA

    def tiles(*count):
        return pltpu.VMEM((*count, side, side), stack.dtype)

    return pl.pallas_call(
        functools.partial(sparse_kernel, row_size, col_size, x_slots, z_slots, 4),
        out_shape=jax.ShapeDtypeStruct(stack.shape, stack.dtype),
        in_specs=[SMEM, VMEM, SMEM],
        out_specs=VMEM,
        scratch_shapes=[
            tiles(slots), tiles(col_size, slots), tiles(slots + X_SLOTS + 2 * Z_SLOTS), tiles(col_size, slots),
            tiles(slots), tiles(slots), tiles(x_slots), tiles(2, z_slots),
            dma((4, chips, slots)), dma((4, chips, slots)), dma((2, x_slots, PARTS)), dma((2, 2, z_slots, PARTS)),
        ],
        compiler_params=pltpu.CompilerParams(collective_id=barrier_id, has_side_effects=True),
        name="sparse",
    )(plan, stack, ids)


def dense_step(mesh, stack, ids, mask):
    row_size, col_size = mesh.shape["row"], mesh.shape["col"]
    length, chips = row_size // 2, col_size // 2
    dma = pltpu.SemaphoreType.DMA
    slots, side, _ = stack.shape
    col_panel = pltpu.VMEM((col_size, slots, side, side), stack.dtype)
    return pl.pallas_call(
        functools.partial(dense_kernel, row_size, col_size),
        out_shape=jax.ShapeDtypeStruct(stack.shape, stack.dtype),
        in_specs=[VMEM, SMEM, SMEM],
        out_specs=VMEM,
        scratch_shapes=[
            col_panel,
            pltpu.VMEM((row_size, slots, side, side), stack.dtype),
            col_panel,
            pltpu.VMEM(stack.shape, stack.dtype),
            pltpu.VMEM(stack.shape, jnp.float32),
            pltpu.VMEM((col_size, 8, 128), jnp.int32),
            pltpu.VMEM((row_size, 8, 128), jnp.int32),
            pltpu.VMEM((8, 128), jnp.int32),
            pltpu.SMEM((col_size, 8, 128), jnp.int32),
            pltpu.SMEM((row_size, 8, 128), jnp.int32),
            dma((4, chips, slots)),
            dma((4, chips, slots)),
            dma((2, 2, length, slots + 2)),
            dma((2, length, slots + 1)),
            dma((2, row_size)),
            dma((2, col_size)),
            dma((2,)),
        ],
        compiler_params=pltpu.CompilerParams(collective_id=0, has_side_effects=True),
        name="purify",
    )(stack, ids, mask)


def solution(mesh):
    def local(tiles, stack_index, block_mask):
        stack, ids = tiles[0, 0], stack_index[0]
        plan = make_plan(mesh, block_mask, stack.shape[0])
        purified = lax.switch(
            plan[7, 0],
            (
                lambda: sparse_step(mesh, X_SLOTS - 1, Z_SLOTS - 1, 1, plan, stack, ids),
                lambda: sparse_step(mesh, X_SLOTS, Z_SLOTS, 2, plan, stack, ids),
                lambda: dense_step(mesh, stack, ids, block_mask),
            ),
        )
        return purified[None, None]

    placed = (P("row", "col", None, None, None), P("row", "col", None), P())
    return jax.shard_map(
        local,
        mesh=mesh,
        in_specs=placed,
        out_specs=P("row", "col", None, None, None),
        check_vma=False,
    )
```

```python
import functools

import jax
import jax.numpy as jnp
from jax import lax
from jax.experimental import pallas as pl
from jax.experimental.pallas import tpu as pltpu
from jax.sharding import PartitionSpec as P
from jax._src.lax.control_flow.conditionals import _switch_internal

MESH = pl.DeviceIdType.MESH
VMEM = pl.BlockSpec(memory_space=pltpu.VMEM)
SMEM = pl.BlockSpec(memory_space=pltpu.SMEM)
HBM = pl.BlockSpec(memory_space=pltpu.HBM)


def send(src, dst, send_sem, recv_sem, row, col):
    return pltpu.make_async_remote_copy(
        src_ref=src,
        dst_ref=dst,
        send_sem=send_sem,
        recv_sem=recv_sem,
        device_id=(row, col),
        device_id_type=MESH,
    )


def greet(row_size, col_size, row, col, with_rows):
    barrier = pltpu.get_barrier_semaphore()
    count = col_size - 1
    for step in range(1, col_size):
        peer = lax.rem(col + step, col_size)
        pl.semaphore_signal(barrier, inc=1, device_id=(row, peer), device_id_type=MESH)
    if with_rows:
        count += row_size - 1
        for step in range(1, row_size):
            peer = lax.rem(row + step, row_size)
            pl.semaphore_signal(barrier, inc=1, device_id=(peer, col), device_id_type=MESH)
    pl.semaphore_wait(barrier, count)


class ColGather:
    def __init__(self, row, col, col_size, slots, own, panel, sems, far=None, far_slots=None):
        self.row, self.col, self.slots = row, col, slots
        self.own, self.panel, self.sems = own, panel, sems
        self.far = own if far is None else far
        self.far_slots = slots if far_slots is None else far_slots
        self.chips = col_size // 2
        self.chip, self.core = col // 2, lax.rem(col, 2)
        self.partner = col + 1 - 2 * self.core

    def across(self, step, slot):
        target = 2 * lax.rem(self.chip + step, self.chips) + self.core
        return send(
            self.far.at[slot], self.panel.at[self.col, slot],
            self.sems.at[0, step - 1, slot], self.sems.at[1, step - 1, slot], self.row, target,
        )

    def beside(self, step, slot):
        origin = 2 * lax.rem(self.chip + self.chips - step, self.chips) + self.core
        src = self.own.at[slot] if step == 0 else self.panel.at[origin, slot]
        return send(
            src, self.panel.at[origin, slot],
            self.sems.at[2, step, slot], self.sems.at[3, step, slot], self.row, self.partner,
        )

    def start(self):
        for slot in range(self.slots):
            for step in range(1, self.chips):
                self.across(step, slot).start()
        for slot in range(self.slots):
            self.beside(0, slot).start()

    def origin(self, step, core):
        return 2 * lax.rem(self.chip + self.chips - step, self.chips) + core

    def forward(self, use=None):
        for slot in range(self.far_slots):
            for step in range(1, self.chips):
                self.across(step, slot).wait_recv()
                self.beside(step, slot).start()
                if use is not None:
                    use(self.origin(step, self.core), slot)

    def count(self, step):
        return self.far_slots if step else self.slots

    def collect(self, use, steps):
        for step in steps:
            for slot in range(self.count(step)):
                self.beside(step, slot).wait_recv()
                if use is not None:
                    use(self.origin(step, 1 - self.core), slot)

    def settle(self):
        for step in range(self.chips):
            for slot in range(self.count(step)):
                if step:
                    self.across(step, slot).wait_send()
                self.beside(step, slot).wait_send()


def dense_kernel(
    row_size, col_size, tiles, ids, mask, out, left, right, squares, square, total, left_ids, right_ids, ids_out,
    left_labels, right_labels, col_sems, square_sems, line_sems, side_sems, row_id_sems, col_id_sems, label_sems,
):
    row, col = lax.axis_index("row"), lax.axis_index("col")
    slots, side = tiles.shape[0], tiles.shape[1]
    half = side // 2
    length = row_size // 2
    place, lane = row // 2, lax.rem(row, 2)
    mate = row + 1 - 2 * lane

    lane_iota = lax.broadcasted_iota(jnp.int32, (8, 128), 1)
    packed = jnp.full((8, 128), -1, jnp.int32)
    for slot in range(slots):
        packed = jnp.where(lane_iota == slot, ids[7, slot], packed)
    ids_out[...] = packed
    greet(row_size, col_size, row, col, True)

    pieces = [(slot, 0, side, False) for slot in range(slots - 1)]
    cut = side * 64 // 256
    pieces += [(slots - 1, cut, side - cut, False)]
    early = (slots - 1, 0, cut, True)
    mine = [early] + pieces
    count = len(mine)

    def view(ref, piece, origin=None):
        slot, first, rows, _ = piece
        if origin is None:
            return ref.at[slot, pl.ds(first, rows)]
        return ref.at[origin, slot, pl.ds(first, rows)]

    def to_mate(index, at):
        piece = mine[index]
        origin = 2 * at + lane
        return send(
            view(right, piece, origin), view(right, piece, origin),
            side_sems.at[0, at, index], side_sems.at[1, at, index], mate, col,
        )

    def own_to_mate(index):
        piece = mine[index]
        return send(
            view(tiles, piece), view(right, piece, row),
            side_sems.at[0, place, index], side_sems.at[1, place, index], mate, col,
        )

    def from_mate(index, at):
        piece = mine[index]
        origin = 2 * at + 1 - lane
        return send(
            view(right, piece, origin), view(right, piece, origin),
            side_sems.at[0, at, index], side_sems.at[1, at, index], mate, col,
        )

    def along(way, step, index, first=False):
        heading = 1 if way == 0 else -1
        piece = mine[0] if index == count else mine[index]
        on_lane = 1 - lane if index == count else lane
        origin = 2 * (place - heading * step) + on_lane
        src = view(tiles, piece) if first and index < count else view(right, piece, origin)
        return send(
            src, view(right, piece, origin),
            line_sems.at[way, 0, step, index], line_sems.at[way, 1, step, index],
            row + 2 * heading, col,
        )

    def landing(way, step, index):
        heading = 1 if way == 0 else -1
        piece = mine[0] if index == count else mine[index]
        on_lane = 1 - lane if index == count else lane
        origin = 2 * (place - heading * (step + 1)) + on_lane
        return send(
            view(right, piece, origin), view(right, piece, origin),
            line_sems.at[way, 0, step, index], line_sems.at[way, 1, step, index],
            row + 2 * heading, col,
        )

    can_send = (place + 1 < length, place > 0)

    def arrives(way, step):
        return place - step >= 1 if way == 0 else place + step + 1 < length

    def goes(way, step):
        if way == 0:
            return (place - step >= 0) & (place + 1 < length)
        return (place + step < length) & (place > 0)

    def id_row(step):
        return send(
            ids_out, right_ids.at[row], row_id_sems.at[0, step], row_id_sems.at[1, step],
            lax.rem(row + step, row_size), col,
        )

    def id_col(step):
        return send(
            ids_out, left_ids.at[col], col_id_sems.at[0, step], col_id_sems.at[1, step],
            row, lax.rem(col + step, col_size),
        )

    for step in range(1, row_size):
        id_row(step).start()
    for step in range(1, col_size):
        id_col(step).start()

    left_gather = ColGather(row, col, col_size, slots, tiles, left, col_sems)
    left_gather.start()
    own_to_mate(0).start()
    for index in range(count):
        for way in range(2):
            @pl.when(can_send[way])
            def _():
                along(way, 0, index, True).start()
        if index:
            own_to_mate(index).start()


    from_mate(0, place).wait_recv()
    for way in range(2):
        @pl.when(can_send[way])
        def _():
            along(way, 0, count).start()

    right[row] = tiles[...]
    left[col] = tiles[...]
    right_ids[row] = packed
    left_ids[col] = packed

    def turn(step, unused):
        for index in list(range(count)) + [count]:
            for way in range(2):
                @pl.when(arrives(way, step))
                def _():
                    landing(way, step, index).wait_recv()

                    @pl.when(can_send[way])
                    def _():
                        along(way, step + 1, index).start()

                    if 0 < index < count:
                        heading = 1 if way == 0 else -1
                        to_mate(index, place - heading * (step + 1)).start()
        return unused

    block_rows, block_cols = mask.shape[0] // row_size, mask.shape[1] // col_size
    owns = []
    for slot in range(slots):
        own = ids[7, slot]
        own_row, own_col = own // block_cols, lax.rem(own, block_cols)
        out_row, out_col = row * block_rows + own_row, col * block_cols + own_col
        owns.append((own_row, own_col, out_row, out_col, mask[out_row, out_col] > 0))

    def find(labels, region, wanted):
        spot, found = jnp.int32(0), labels[region, 0, 0] == wanted
        for other in range(1, slots):
            same = labels[region, 0, other] == wanted
            spot = jnp.where(same, other, spot)
            found = found | same
        return spot, found

    def square_term(origin, place):
        label = right_labels[origin, 0, place]
        inner = origin * block_rows + label // block_cols
        band = inner // block_cols
        chosen = []
        for own_row, own_col, out_row, out_col, live in owns:
            spot, found = find(left_labels, band, own_row * block_cols + lax.rem(inner, block_cols))
            use = live & found & (lax.rem(label, block_cols) == own_col)
            use = use & (mask[out_row, inner] > 0) & (mask[inner, out_col] > 0)
            tile = left[band, spot]
            chosen.append(jnp.where(use, tile, jnp.zeros_like(tile)))
        term = jnp.dot(
            jnp.concatenate(chosen, axis=0), right[origin, place], preferred_element_type=jnp.float32
        )
        total[...] += term.reshape(total.shape)

    def cube_term(origin, place):
        label = left_labels[origin, 0, place]
        inner = origin * block_cols + lax.rem(label, block_cols)
        band = inner // block_rows
        piece = squares[origin, place]
        for slot, (own_row, own_col, out_row, out_col, live) in enumerate(owns):
            spot, found = find(right_labels, band, lax.rem(inner, block_rows) * block_cols + own_col)
            use = live & found & (label // block_cols == own_row)
            use = use & (mask[out_row, inner] > 0) & (mask[inner, out_col] > 0)
            tile = right[band, spot]
            total[slot] += jnp.dot(
                piece, jnp.where(use, tile, jnp.zeros_like(tile)), preferred_element_type=jnp.float32
            )

    def stack_terms(origin, wait=None):
        for slot in range(slots):
            if wait is not None:
                wait(slot)
            square_term(origin, slot)

    def mate_terms(at):
        stack_terms(2 * at + 1 - lane, lambda slot: from_mate(slot + 1, at).wait_recv())

    def consume(step):
        for way in range(2):
            @pl.when(arrives(way, step))
            def _():
                heading = 1 if way == 0 else -1
                stack_terms(2 * (place - heading * (step + 1)) + lane)
        for way in range(2):
            @pl.when(arrives(way, step))
            def _():
                heading = 1 if way == 0 else -1
                mate_terms(place - heading * (step + 1))

    total[...] = jnp.zeros_like(total)
    turn(0, 0)
    for step in range(1, row_size):
        id_row(step).wait()
    for step in range(1, col_size):
        id_col(step).wait()
    copies = (
        pltpu.make_async_copy(left_ids, left_labels, label_sems.at[0]),
        pltpu.make_async_copy(right_ids, right_labels, label_sems.at[1]),
    )
    for copy in copies:
        copy.start()
    for copy in copies:
        copy.wait()
    left_gather.forward()
    left_gather.collect(None, range(left_gather.chips))
    stack_terms(row)
    mate_terms(place)

    def advance(step, unused):
        turn(step, 0)
        consume(step - 1)
        return unused

    lax.fori_loop(1, length - 1, advance, 0)
    consume(length - 2)

    square[...] = total[...].astype(square.dtype)

    square_gather = ColGather(row, col, col_size, slots, square, squares, square_sems)

    def keep(slot, unused):
        squares[col, slot] = square[slot]
        for step in range(1, square_gather.chips):
            square_gather.across(step, slot).start()
        square_gather.beside(0, slot).start()
        return unused

    lax.fori_loop(0, slots, keep, 0)
    total[...] = jnp.zeros_like(total)
    for slot in range(slots):
        cube_term(col, slot)
    square_gather.collect(cube_term, [0])
    square_gather.forward(cube_term)
    square_gather.collect(cube_term, range(1, square_gather.chips))
    out[...] = (3.0 * square[...].astype(jnp.float32) - 2.0 * total[...]).astype(out.dtype)

    left_gather.settle()
    square_gather.settle()

    def settle(step, unused):
        for index in range(count + 1):
            for way in range(2):
                @pl.when(goes(way, step))
                def _():
                    along(way, step, index).wait_send()
        return unused

    lax.fori_loop(0, length - 1, settle, 0)
    own_to_mate(0).wait_send()

    def collect(at, unused):
        for index in range(1, count):
            to_mate(index, at).wait_send()
        return unused

    lax.fori_loop(0, length, collect, 0)

X_SLOTS = 3
Z_SLOTS = 5
Y_SLOTS = 2
TERMS = 4
PARTS = 4
F32, BF16 = jnp.float32, jnp.bfloat16


def iota(shape, axis):
    return lax.broadcasted_iota(jnp.int32, shape, axis)


def plan_kernel(
    row_size, col_size, slots, far_ids, far_mask, far_tiles, out, choice, canon, x_out, ids, mask, tiles, tile_row,
    tile_col, tile_spot, reach, ranges, table, across, stops, sems,
):
    fetches = [
        pltpu.make_async_copy(src, dst, sems.at[number])
        for number, (src, dst) in enumerate(((far_mask, mask), (far_ids, ids), (far_tiles, tiles)))
    ]
    for fetch in fetches:
        fetch.start()
    blocks, lanes = mask.shape[0], 128
    block_rows, block_cols = blocks // row_size, blocks // col_size
    length = row_size // 2
    lines = 4 * col_size
    row, col = lax.axis_index("row"), lax.axis_index("col")
    place, lane = row // 2, lax.rem(row, 2)
    dot = functools.partial(jnp.dot, preferred_element_type=F32)

    fetches[0].wait()
    occupied = mask[...].astype(F32)
    grid = occupied.astype(BF16)
    row_of, lane_of = iota((blocks, lanes), 0), iota((blocks, lanes), 1)
    spread = row_of - lax.rem(lane_of, block_cols)
    keep = lax.rem(row_of, block_rows) == lane_of // block_cols
    before = (iota((lanes, lanes), 0) <= iota((lanes, lanes), 1)).astype(F32).astype(BF16)
    region_of, spot_of = iota((row_size, lanes), 0), iota((row_size, lanes), 1)
    home = spot_of // slots
    tile_home = iota((1, lanes), 1) // slots
    spot_value = (spot_of + 1).astype(F32)
    at = row_of.astype(F32)

    def groups(value):
        return jnp.sum(value.reshape(row_size, block_rows, lanes), axis=1)

    for panel in range(col_size):
        pick = (spread == panel * block_cols).astype(F32).astype(BF16)
        flat = groups(jnp.where(keep, dot(grid, pick), 0.0))
        rank = dot(flat.astype(BF16), before)
        spots = jnp.zeros((row_size, lanes), F32)
        for slot in range(slots):
            found = jnp.where((rank == slot + 1) & (flat > 0), spot_value, 0.0)
            found = jnp.sum(found, axis=1, keepdims=True)
            spots = jnp.where(spot_of == region_of * slots + slot, found, spots)
        spot = jnp.sum(spots, axis=0, keepdims=True) - 1.0
        high = jnp.floor((spot + 0.5) / block_cols)
        block_row = jnp.where(spot >= 0, tile_home.astype(F32) * block_rows + high, -1.0)
        block_col = jnp.where(spot >= 0, panel * block_cols + spot - high * block_cols, -1.0)
        tile_spot[pl.ds(panel, 1), :] = spot
        tile_row[pl.ds(panel, 1), :] = block_row
        tile_col[pl.ds(panel, 1), :] = block_col
        by_row = dot(grid, (at == block_row).astype(F32).astype(BF16))
        by_col = dot(grid, (at == block_col).astype(F32).astype(BF16))
        wanted = (groups(by_row * by_col) > 0) & (region_of != home)
        for side in range(2):
            for way in range(2):
                step = region_of // 2 + 1 if way == 0 else length - region_of // 2
                far = jnp.where(wanted & (lax.rem(region_of, 2) == side), step.astype(F32), 0.0)
                reach[pl.ds((side * 2 + way) * col_size + panel, 1), :] = jnp.max(far, axis=0, keepdims=True)
            gap = jnp.abs(region_of // 2 - home // 2) + 1
            gap = jnp.where(wanted & (lax.rem(region_of, 2) == side), gap.astype(F32), 0.0)
            gap = jnp.max(gap, axis=0, keepdims=True)
            for way in range(2):
                ranges[pl.ds((side * 2 + way) * col_size + panel, 1), :] = gap

    far = reach[...]
    line, tile = iota((lines, lanes), 0), iota((lines, lanes), 1)
    side, way = line // (2 * col_size), lax.rem(line // col_size, 2)
    origin, number = tile // slots, lax.rem(tile, slots)
    begin = jnp.where(way == 0, origin // 2, length - 1 - origin // 2)
    begin = jnp.minimum(begin, jnp.where(tile < row_size * slots, begin, length))
    straight = lax.rem(origin, 2) == side
    crosses = (ranges[...] > 0) & jnp.logical_not(straight)
    value = jnp.where(crosses, ranges[...] * 8 - number.astype(F32), -8.0)
    order = jnp.zeros((lines, lanes), F32)
    for back in range(1, slots):
        order += jnp.where((number >= back) & (pltpu.roll(value, back, 1) > value), 1.0, 0.0)
        order += jnp.where((number + back < slots) & (pltpu.roll(value, lanes - back, 1) > value), 1.0, 0.0)
    across[...] = jnp.where(crosses, order + 1.0, 0.0)
    trouble = jnp.zeros((lines, lanes), F32)
    rank_value = (128 * tile).astype(F32)
    table_now = jnp.zeros((lines, lanes), F32)
    stop = jnp.zeros((lines, lanes), F32)
    number_value = number.astype(F32)
    for step in range(length - 1):
        fresh = begin == step
        ready = jnp.where(fresh, jnp.where(straight, 0.0, order + 1.0), stop + 1.0)
        code = jnp.where(
            fresh, jnp.where(straight, number_value, slots + order), slots + X_SLOTS + stop
        )
        left = jnp.where((far > step + 1) & (begin <= step), 1.0, 0.0)
        key = far * (128 * 128) - rank_value + code + 1.0
        for turn in range(Z_SLOTS):
            live = jnp.where((left > 0) & (ready <= turn), key, 0.0)
            best = jnp.max(live, axis=1, keepdims=True)
            taken = (live == best) & (live > 0)
            stop = jnp.where(taken, float(turn), stop)
            left = jnp.where(taken, 0.0, left)
            table_now = jnp.where(tile == step * 8 + turn, best, table_now)
            if turn == Z_SLOTS - 2:
                trouble = jnp.maximum(trouble, left)
        trouble = jnp.maximum(trouble, 2.0 * left)
        stops[step] = stop
    table_now = table_now - 128 * jnp.floor(table_now / 128)
    table[...] = jnp.maximum(table_now - 1.0, 0.0)

    here, there = (lane * 2) * col_size + col, (lane * 2 + 1) * col_size + col
    other = (1 - lane) * 2 * col_size + col
    tile, tile_number = iota((1, lanes), 1), lax.rem(iota((1, lanes), 1), slots)
    tile_place = tile_home // 2
    my_rows, my_cols = tile_row[pl.ds(col, 1), :], tile_col[pl.ds(col, 1), :]
    beyond = stops[jnp.maximum(place - 1, 0), pl.ds(here, 1), :]
    under = stops[jnp.maximum(length - 2 - place, 0), pl.ds(there, 1), :]
    spot = jnp.where(tile_place < place, slots + X_SLOTS + beyond, slots + X_SLOTS + Z_SLOTS + under)
    spot = jnp.where(tile_place == place, slots - 1 + across[pl.ds(here, 1), :], spot)
    spot = jnp.where(tile_home == row, tile_number.astype(F32), spot)

    inside = iota((blocks, blocks), 0), iota((blocks, blocks), 1)
    same_rows = inside[0] // block_rows == inside[1] // block_rows
    same_cols = inside[0] // block_cols == inside[1] // block_cols
    lower = (same_rows & (inside[1] < inside[0])).astype(F32).astype(BF16)
    whole = same_cols.astype(F32).astype(BF16)
    upper = (same_cols & (inside[0] < inside[1])).astype(F32).astype(BF16)
    chip_of = inside[1] // (2 * block_cols)
    flipped = occupied.T.astype(BF16)
    shared = dot(grid, flipped)
    inner = jnp.zeros((blocks, blocks), F32)
    for chip in range(col_size // 2):
        on_chip = jnp.where(chip_of == chip, occupied, 0.0).astype(BF16)
        inner = jnp.where(chip_of == chip, dot(on_chip, flipped), inner)
    leaves = jnp.where((occupied > 0) & (shared > inner), 1.0, 0.0)
    gone = leaves.astype(BF16)
    ranks = dot(dot(lower, grid).astype(BF16), whole) + dot(grid, upper)
    y_ranks = dot(dot(lower, gone).astype(BF16), whole) + dot(gone, upper)
    panels = ((inside[1] // block_cols) * slots).astype(F32)
    labels = ranks + panels
    y_labels = jnp.where(chip_of == col // 2, ranks, y_ranks) + panels
    y_order = leaves * (y_ranks + 1.0)

    def peak(value):
        return jnp.max(jnp.max(value, axis=1, keepdims=True), axis=0, keepdims=True)

    fan = peak(dot(grid, grid) * occupied)
    crowd = peak(y_order)

    chosen = (at == my_rows).astype(F32).astype(BF16)
    met = dot(grid, chosen)
    named, y_named = dot(labels.astype(BF16), chosen), dot(y_labels.astype(BF16), chosen)
    sub, column = iota((8, lanes), 0), iota((8, lanes), 1)
    pairs = jnp.zeros((8, lanes), F32)
    fetches[1].wait()
    result = jnp.where(sub == 0, table[pl.ds(here, 1), :], 0.0)
    result = jnp.where(sub == 1, table[pl.ds(there, 1), :], result)
    inside_rows, inside_cols = inside[0].astype(F32), inside[1].astype(F32)
    for slot in range(slots):
        mine = tile == row * slots + slot
        out_row = jnp.sum(jnp.where(mine, my_rows, 0.0), axis=1, keepdims=True)
        out_col = jnp.sum(jnp.where(mine, my_cols, 0.0), axis=1, keepdims=True)
        on_row = at == out_row
        joins = jnp.sum(jnp.where(on_row, met, 0.0), axis=0, keepdims=True)
        name = jnp.sum(jnp.where(on_row, named, 0.0), axis=0, keepdims=True)
        y_name = jnp.sum(jnp.where(on_row, y_named, 0.0), axis=0, keepdims=True)
        use = (joins > 0) & (my_cols == out_col) & (my_rows >= 0)
        pairs = jnp.where((sub == slot) & use, name * 64 + spot + 1, pairs)
        pairs = jnp.where((sub == slot + slots) & use, y_name * 64 + spot + 1, pairs)
        y_spot = jnp.where((inside_rows == out_row) & (inside_cols == out_col), y_order, 0.0)
        y_spot = jnp.sum(jnp.sum(y_spot, axis=1, keepdims=True), axis=0, keepdims=True)
        result = jnp.where((sub == 6) & (column == 8 + slot), y_spot, result)
    product = jnp.zeros((8, lanes), F32)
    shifted = column - jnp.where(sub >= slots, 16, 0)
    for term in range(TERMS):
        best = jnp.max(pairs, axis=1, keepdims=True)
        pairs = jnp.where(pairs == best, 0.0, pairs)
        product = jnp.where(shifted == term, best, product)

    level = peak(trouble) * 2.0
    level = jnp.where(fan > TERMS, 4.0, level) + jnp.where((level < 4) & (fan <= TERMS) & (crowd > Y_SLOTS), 1.0, 0.0)
    choice[...] = level.astype(jnp.int32)
    for slot in range(slots):
        mine = (tile_home == row) & (tile_spot[pl.ds(col, 1), :] == ids[0, slot].astype(F32))
        match = jnp.sum(jnp.where(mine, tile_number.astype(F32) + 1.0, 0.0), axis=1, keepdims=True)
        order = jnp.where(tile == row * slots + slot, across[pl.ds(other, 1), :], 0.0)
        order = jnp.sum(order, axis=1, keepdims=True)
        result = jnp.where((sub == 6) & (column == slot), match, result)
        result = jnp.where((sub == 2) & (column == slot), order, result)
        result = jnp.where((sub == 7) & (column == slot), ids[0, slot].astype(F32), result)
        both = jnp.where((sub == slot) | (sub == slot + slots), product, 0.0)
        result = jnp.where(sub == 3 + slot, jnp.sum(both, axis=0, keepdims=True), result)
    out[...] = result.astype(jnp.int32)

    fetches[2].wait()
    held = [[result[6:7, slot : slot + 1] == number + 1 for slot in range(slots)] for number in range(slots)]
    for number in range(slots):
        piece = jnp.zeros(tiles.shape[1:], tiles.dtype)
        for slot in range(slots):
            piece = jnp.where(held[number][slot], tiles[slot], piece)
        canon[number] = piece
    for slot in range(slots):
        piece = canon[0]
        for number in range(1, slots):
            piece = jnp.where(result[2:3, number : number + 1] == slot + 1, canon[number], piece)
        x_out[slot] = piece


def make_plan(mesh, ids, mask, stack):
    row_size, col_size = mesh.shape["row"], mesh.shape["col"]
    slots = ids.shape[1]
    panel = pltpu.VMEM((col_size, 128), F32)
    lines = (4 * col_size, 128)
    return pl.pallas_call(
        functools.partial(plan_kernel, row_size, col_size, slots),
        out_shape=(
            jax.ShapeDtypeStruct((8, 128), jnp.int32),
            jax.ShapeDtypeStruct((1, 1), jnp.int32),
            jax.ShapeDtypeStruct(stack.shape, stack.dtype),
            jax.ShapeDtypeStruct(stack.shape, stack.dtype),
        ),
        in_specs=[HBM, HBM, HBM],
        out_specs=(VMEM, VMEM, VMEM, VMEM),
        scratch_shapes=[
            pltpu.SMEM(ids.shape, ids.dtype), pltpu.VMEM(mask.shape, mask.dtype), pltpu.VMEM(stack.shape, stack.dtype),
            panel, panel, panel, *[pltpu.VMEM(lines, F32)] * 4, pltpu.VMEM((row_size // 2 - 1, *lines), F32),
            pltpu.SemaphoreType.DMA((3,)),
        ],
        compiler_params=pltpu.CompilerParams(vmem_limit_bytes=16 * 2**20),
        name="plan",
    )(ids, mask, stack)


def sparse_kernel(
    row_size, col_size, z_slots, y_slots, plan, canon, x_out, out, left, held, squares, square, final,
    y_out, z_out, col_sems, square_sems, x_sems, z_sems,
):
    row, col = lax.axis_index("row"), lax.axis_index("col")
    slots, side = canon.shape[0], canon.shape[1]
    rows = side // PARTS
    length = row_size // 2
    place, lane = row // 2, lax.rem(row, 2)
    mate = row + 1 - 2 * lane
    chips = col_size // 2
    chip, core = col // 2, lax.rem(col, 2)
    x_slots = slots

    barrier = pltpu.get_barrier_semaphore()

    def hello(to_row, to_col):
        pl.semaphore_signal(barrier, inc=1, device_id=(to_row, to_col), device_id_type=MESH)

    hello(mate, col)
    hello(row, col + 1 - 2 * core)
    for step in range(1, chips):
        hello(row, 2 * lax.rem(chip + step, chips) + core)
    for way in range(2):
        @pl.when((place + 1 < length) if way == 0 else (place > 0))
        def _():
            hello(row + 2 - 4 * way, col)

    ends = jnp.where(place == 0, 1, 0) + jnp.where(place + 1 == length, 1, 0)
    pl.semaphore_wait(barrier, 2 + chips - 1 + 2 - ends)

    def x_copy(slot, part):
        span = pl.ds(part * rows, rows)
        return send(
            x_out.at[slot, span], held.at[slots + slot, span],
            x_sems.at[0, slot, part], x_sems.at[1, slot, part], mate, col,
        )

    def z_copy(way, slot, part):
        span = pl.ds(part * rows, rows)
        return send(
            z_out.at[way, slot, span], held.at[slots + X_SLOTS + way * Z_SLOTS + slot, span],
            z_sems.at[way, 0, slot, part], z_sems.at[way, 1, slot, part], row + 2 - 4 * way, col,
        )

    for slot in range(x_slots):
        for part in range(PARTS):
            x_copy(slot, part).start()
    left_gather = ColGather(row, col, col_size, slots, canon, left, col_sems)
    left_gather.start()

    done = (place, length - 1 - place)
    for slot in range(z_slots):
        for way in range(2):
            @pl.when(done[way] + 1 < length)
            def _():
                code = plan[way, done[way] * 8 + slot]
                tile = canon[0]
                for number in range(1, slots):
                    tile = jnp.where(code == number, canon[number], tile)
                for other in range(min(slot - 1, x_slots)):
                    tile = jnp.where(code == slots + other, held[slots + other], tile)
                for other in range(slot - 1):
                    spot = X_SLOTS + slots + other
                    tile = jnp.where(code == spot, held[spot + way * Z_SLOTS], tile)
                z_out[way, slot] = tile

        for part in range(PARTS):
            span = pl.ds(part * rows, rows)
            if 1 <= slot <= x_slots:
                x_copy(slot - 1, part).wait_recv()
            for way in range(2):
                @pl.when(done[way] + 1 < length)
                def _():
                    if slot:
                        @pl.when(done[way] > 0)
                        def _():
                            z_copy(way, slot - 1, part).wait_recv()

                        code = plan[way, done[way] * 8 + slot]
                        piece = z_out[way, slot, span]
                        if slot <= x_slots:
                            piece = jnp.where(code == slots + slot - 1, held[slots + slot - 1, span], piece)
                        spot = X_SLOTS + slots + slot - 1
                        piece = jnp.where(code == spot, held[spot + way * Z_SLOTS, span], piece)
                        z_out[way, slot, span] = piece
                    z_copy(way, slot, part).start()

    left_gather.forward()
    for number in range(slots):
        held[number] = canon[number]
        left[col, number] = canon[number]

    for slot in range(z_slots - 1, x_slots):
        for part in range(PARTS):
            x_copy(slot, part).wait_recv()
    for way in range(2):
        @pl.when(done[way] + 1 == length)
        def _():
            for slot in range(z_slots - 1):
                for part in range(PARTS):
                    z_copy(way, slot, part).wait_recv()

        @pl.when(done[way] > 0)
        def _():
            for part in range(PARTS):
                z_copy(way, z_slots - 1, part).wait_recv()

    left_gather.collect(None, range(left_gather.chips))

    def sum_terms(panel, number, first):
        total = jnp.zeros((side, side), F32)
        for term in range(TERMS):
            code = plan[3 + number, first + term]
            pair = jnp.maximum(code - 1, 0)
            name, spot = pair // 64, lax.rem(pair, 64)
            tile = panel[name // slots, lax.rem(name, slots)]
            total += jnp.dot(
                jnp.where(code > 0, tile, jnp.zeros_like(tile)), held[spot], preferred_element_type=F32
            )
        return total

    square_gather = ColGather(row, col, col_size, slots, square, squares, square_sems, y_out, y_slots)

    for slot in range(y_slots):
        number = jnp.int32(0)
        for other in range(1, slots):
            number = jnp.where(plan[6, 8 + other] == slot + 1, other, number)
        y_out[slot] = sum_terms(left, number, 0).astype(square.dtype)
        for step in range(1, chips):
            square_gather.across(step, slot).start()

    def first(number, unused):
        tile = sum_terms(left, number, 0).astype(square.dtype)
        square[number] = tile
        squares[col, number] = tile
        square_gather.beside(0, number).start()
        return unused

    lax.fori_loop(0, slots, first, 0)
    square_gather.forward()
    square_gather.collect(None, range(chips))

    def second(number, unused):
        final[number] = (3.0 * square[number].astype(F32) - 2.0 * sum_terms(squares, number, 16)).astype(final.dtype)
        return unused

    lax.fori_loop(0, slots, second, 0)
    for slot in range(slots):
        tile = jnp.zeros((side, side), out.dtype)
        for number in range(slots):
            tile = jnp.where(plan[6, slot] == number + 1, final[number], tile)
        out[slot] = tile

    left_gather.settle()
    square_gather.settle()

    for part in range(PARTS):
        for slot in range(x_slots):
            x_copy(slot, part).wait_send()
    for way in range(2):
        @pl.when(done[way] + 1 < length)
        def _():
            for slot in range(z_slots):
                for part in range(PARTS):
                    z_copy(way, slot, part).wait_send()


def room(panels, slots, side):
    return (4 * panels + 16) * slots * side * side * 2 + 8 * 2**20


def sparse_step(mesh, z_slots, y_slots, barrier_id, plan, stack, x_stack):
    row_size, col_size = mesh.shape["row"], mesh.shape["col"]
    chips = col_size // 2
    slots, side, _ = stack.shape
    dma = pltpu.SemaphoreType.DMA

    def tiles(*count):
        return pltpu.VMEM((*count, side, side), stack.dtype)

    return pl.pallas_call(
        functools.partial(sparse_kernel, row_size, col_size, z_slots, y_slots),
        out_shape=jax.ShapeDtypeStruct(stack.shape, stack.dtype),
        in_specs=[SMEM, VMEM, VMEM],
        out_specs=VMEM,
        scratch_shapes=[
            tiles(col_size, slots), tiles(slots + X_SLOTS + 2 * Z_SLOTS), tiles(col_size, slots),
            tiles(slots), tiles(slots), tiles(y_slots), tiles(2, z_slots),
            dma((4, chips, slots)), dma((4, chips, slots)), dma((2, slots, PARTS)), dma((2, 2, z_slots, PARTS)),
        ],
        compiler_params=pltpu.CompilerParams(
            collective_id=barrier_id, has_side_effects=True, vmem_limit_bytes=room(col_size, slots, side)
        ),
        name="sparse",
    )(plan, stack, x_stack)


def dense_step(mesh, plan, stack, mask):
    row_size, col_size = mesh.shape["row"], mesh.shape["col"]
    length, chips = row_size // 2, col_size // 2
    dma = pltpu.SemaphoreType.DMA
    slots, side, _ = stack.shape
    col_panel = pltpu.VMEM((col_size, slots, side, side), stack.dtype)
    return pl.pallas_call(
        functools.partial(dense_kernel, row_size, col_size),
        out_shape=jax.ShapeDtypeStruct(stack.shape, stack.dtype),
        in_specs=[VMEM, SMEM, SMEM],
        out_specs=VMEM,
        scratch_shapes=[
            col_panel,
            pltpu.VMEM((row_size, slots, side, side), stack.dtype),
            col_panel,
            pltpu.VMEM(stack.shape, stack.dtype),
            pltpu.VMEM(stack.shape, jnp.float32),
            pltpu.VMEM((col_size, 8, 128), jnp.int32),
            pltpu.VMEM((row_size, 8, 128), jnp.int32),
            pltpu.VMEM((8, 128), jnp.int32),
            pltpu.SMEM((col_size, 8, 128), jnp.int32),
            pltpu.SMEM((row_size, 8, 128), jnp.int32),
            dma((4, chips, slots)),
            dma((4, chips, slots)),
            dma((2, 2, length, slots + 2)),
            dma((2, length, slots + 1)),
            dma((2, row_size)),
            dma((2, col_size)),
            dma((2,)),
        ],
        compiler_params=pltpu.CompilerParams(
            collective_id=0, has_side_effects=True, vmem_limit_bytes=room(row_size + col_size, slots, side)
        ),
        name="purify",
    )(stack, plan, mask)


def solution(mesh):
    def local(tiles, stack_index, block_mask):
        stack = tiles[0, 0]
        plan, choice, canon, crossing = make_plan(mesh, stack_index[0], block_mask, stack)
        branches = [
            functools.partial(sparse_step, mesh, z_slots, y_slots, 1 + 2 * (z_slots == Z_SLOTS) + (y_slots > Y_SLOTS))
            for z_slots in (Z_SLOTS - 1, Z_SLOTS) for y_slots in (Y_SLOTS, stack.shape[0])
        ]
        branches = [lambda branch=branch: branch(plan, canon, crossing) for branch in branches]
        branches.append(lambda: dense_step(mesh, plan, stack, block_mask))
        purified = _switch_internal(choice[0, 0], branches, (), branches_platforms=None)
        return purified[None, None]

    placed = (P("row", "col", None, None, None), P("row", "col", None), P())
    return jax.shard_map(
        local,
        mesh=mesh,
        in_specs=placed,
        out_specs=P("row", "col", None, None, None),
        check_vma=False,
    )
```

```python
import functools

import jax
import jax.numpy as jnp
from jax import lax
from jax.experimental import pallas as pl
from jax.experimental.pallas import tpu as pltpu
from jax.sharding import PartitionSpec as P
from jax._src.lax.control_flow.conditionals import _switch_internal

MESH = pl.DeviceIdType.MESH
VMEM = pl.BlockSpec(memory_space=pltpu.VMEM)
SMEM = pl.BlockSpec(memory_space=pltpu.SMEM)
HBM = pl.BlockSpec(memory_space=pltpu.HBM)


def send(src, dst, send_sem, recv_sem, row, col):
    return pltpu.make_async_remote_copy(
        src_ref=src,
        dst_ref=dst,
        send_sem=send_sem,
        recv_sem=recv_sem,
        device_id=(row, col),
        device_id_type=MESH,
    )


def greet(row_size, col_size, row, col, with_rows):
    barrier = pltpu.get_barrier_semaphore()
    count = col_size - 1
    for step in range(1, col_size):
        peer = lax.rem(col + step, col_size)
        pl.semaphore_signal(barrier, inc=1, device_id=(row, peer), device_id_type=MESH)
    if with_rows:
        count += row_size - 1
        for step in range(1, row_size):
            peer = lax.rem(row + step, row_size)
            pl.semaphore_signal(barrier, inc=1, device_id=(peer, col), device_id_type=MESH)
    pl.semaphore_wait(barrier, count)


class ColGather:
    def __init__(self, row, col, col_size, slots, own, panel, sems, far=None, far_slots=None, near=None):
        self.row, self.col, self.slots = row, col, slots
        self.own, self.panel, self.sems = own, panel, sems
        self.far, self.near = own if far is None else far, near
        self.far_slots = slots if far_slots is None else far_slots
        self.chips = col_size // 2
        self.chip, self.core = col // 2, lax.rem(col, 2)
        self.partner = col + 1 - 2 * self.core

    def across(self, step, slot):
        target = 2 * lax.rem(self.chip + step, self.chips) + self.core
        return send(
            self.far.at[slot], self.panel.at[self.col, slot],
            self.sems.at[0, step - 1, slot], self.sems.at[1, step - 1, slot], self.row, target,
        )

    def beside(self, step, slot):
        origin = 2 * lax.rem(self.chip + self.chips - step, self.chips) + self.core
        src = self.own.at[slot] if step == 0 else self.panel.at[origin, slot]
        near = self.near is not None and step == 0
        return send(
            src, self.near.at[self.core, slot] if near else self.panel.at[origin, slot],
            self.sems.at[2, step, slot], self.sems.at[3, step, slot], self.row, self.partner,
        )

    def start(self):
        for slot in range(self.slots):
            for step in range(1, self.chips):
                self.across(step, slot).start()
        for slot in range(self.slots):
            self.beside(0, slot).start()

    def origin(self, step, core):
        return 2 * lax.rem(self.chip + self.chips - step, self.chips) + core

    def forward(self, use=None):
        for slot in range(self.far_slots):
            for step in range(1, self.chips):
                self.across(step, slot).wait_recv()
                self.beside(step, slot).start()
                if use is not None:
                    use(self.origin(step, self.core), slot)

    def count(self, step):
        return self.far_slots if step else self.slots

    def collect(self, use, steps):
        for step in steps:
            for slot in range(self.count(step)):
                self.beside(step, slot).wait_recv()
                if use is not None:
                    use(self.origin(step, 1 - self.core), slot)

    def settle(self):
        for step in range(self.chips):
            for slot in range(self.count(step)):
                if step:
                    self.across(step, slot).wait_send()
                self.beside(step, slot).wait_send()


def dense_kernel(
    row_size, col_size, tiles, ids, mask, out, left, right, squares, square, total, left_ids, right_ids, ids_out,
    left_labels, right_labels, col_sems, square_sems, line_sems, side_sems, row_id_sems, col_id_sems, label_sems,
):
    row, col = lax.axis_index("row"), lax.axis_index("col")
    slots, side = tiles.shape[0], tiles.shape[1]
    half = side // 2
    length = row_size // 2
    place, lane = row // 2, lax.rem(row, 2)
    mate = row + 1 - 2 * lane

    lane_iota = lax.broadcasted_iota(jnp.int32, (8, 128), 1)
    packed = jnp.full((8, 128), -1, jnp.int32)
    for slot in range(slots):
        packed = jnp.where(lane_iota == slot, ids[0, slot], packed)
    ids_out[...] = packed
    greet(row_size, col_size, row, col, True)

    pieces = [(slot, 0, side, False) for slot in range(slots - 1)]
    cut = side * 64 // 256
    pieces += [(slots - 1, cut, side - cut, False)]
    early = (slots - 1, 0, cut, True)
    mine = [early] + pieces
    count = len(mine)

    def view(ref, piece, origin=None):
        slot, first, rows, _ = piece
        if origin is None:
            return ref.at[slot, pl.ds(first, rows)]
        return ref.at[origin, slot, pl.ds(first, rows)]

    def to_mate(index, at):
        piece = mine[index]
        origin = 2 * at + lane
        return send(
            view(right, piece, origin), view(right, piece, origin),
            side_sems.at[0, at, index], side_sems.at[1, at, index], mate, col,
        )

    def own_to_mate(index):
        piece = mine[index]
        return send(
            view(tiles, piece), view(right, piece, row),
            side_sems.at[0, place, index], side_sems.at[1, place, index], mate, col,
        )

    def from_mate(index, at):
        piece = mine[index]
        origin = 2 * at + 1 - lane
        return send(
            view(right, piece, origin), view(right, piece, origin),
            side_sems.at[0, at, index], side_sems.at[1, at, index], mate, col,
        )

    def along(way, step, index, first=False):
        heading = 1 if way == 0 else -1
        piece = mine[0] if index == count else mine[index]
        on_lane = 1 - lane if index == count else lane
        origin = 2 * (place - heading * step) + on_lane
        src = view(tiles, piece) if first and index < count else view(right, piece, origin)
        return send(
            src, view(right, piece, origin),
            line_sems.at[way, 0, step, index], line_sems.at[way, 1, step, index],
            row + 2 * heading, col,
        )

    def landing(way, step, index):
        heading = 1 if way == 0 else -1
        piece = mine[0] if index == count else mine[index]
        on_lane = 1 - lane if index == count else lane
        origin = 2 * (place - heading * (step + 1)) + on_lane
        return send(
            view(right, piece, origin), view(right, piece, origin),
            line_sems.at[way, 0, step, index], line_sems.at[way, 1, step, index],
            row + 2 * heading, col,
        )

    can_send = (place + 1 < length, place > 0)

    def arrives(way, step):
        return place - step >= 1 if way == 0 else place + step + 1 < length

    def goes(way, step):
        if way == 0:
            return (place - step >= 0) & (place + 1 < length)
        return (place + step < length) & (place > 0)

    def id_row(step):
        return send(
            ids_out, right_ids.at[row], row_id_sems.at[0, step], row_id_sems.at[1, step],
            lax.rem(row + step, row_size), col,
        )

    def id_col(step):
        return send(
            ids_out, left_ids.at[col], col_id_sems.at[0, step], col_id_sems.at[1, step],
            row, lax.rem(col + step, col_size),
        )

    for step in range(1, row_size):
        id_row(step).start()
    for step in range(1, col_size):
        id_col(step).start()

    left_gather = ColGather(row, col, col_size, slots, tiles, left, col_sems)
    left_gather.start()
    own_to_mate(0).start()
    for index in range(count):
        for way in range(2):
            @pl.when(can_send[way])
            def _():
                along(way, 0, index, True).start()
        if index:
            own_to_mate(index).start()


    from_mate(0, place).wait_recv()
    for way in range(2):
        @pl.when(can_send[way])
        def _():
            along(way, 0, count).start()

    right[row] = tiles[...]
    left[col] = tiles[...]
    right_ids[row] = packed
    left_ids[col] = packed

    def turn(step, unused):
        for index in list(range(count)) + [count]:
            for way in range(2):
                @pl.when(arrives(way, step))
                def _():
                    landing(way, step, index).wait_recv()

                    @pl.when(can_send[way])
                    def _():
                        along(way, step + 1, index).start()

                    if 0 < index < count:
                        heading = 1 if way == 0 else -1
                        to_mate(index, place - heading * (step + 1)).start()
        return unused

    block_rows, block_cols = mask.shape[0] // row_size, mask.shape[1] // col_size
    owns = []
    for slot in range(slots):
        own = ids[0, slot]
        own_row, own_col = own // block_cols, lax.rem(own, block_cols)
        out_row, out_col = row * block_rows + own_row, col * block_cols + own_col
        owns.append((own_row, own_col, out_row, out_col, mask[out_row, out_col] > 0))

    def find(labels, region, wanted):
        spot, found = jnp.int32(0), labels[region, 0, 0] == wanted
        for other in range(1, slots):
            same = labels[region, 0, other] == wanted
            spot = jnp.where(same, other, spot)
            found = found | same
        return spot, found

    def square_term(origin, place):
        label = right_labels[origin, 0, place]
        inner = origin * block_rows + label // block_cols
        band = inner // block_cols
        chosen = []
        for own_row, own_col, out_row, out_col, live in owns:
            spot, found = find(left_labels, band, own_row * block_cols + lax.rem(inner, block_cols))
            use = live & found & (lax.rem(label, block_cols) == own_col)
            use = use & (mask[out_row, inner] > 0) & (mask[inner, out_col] > 0)
            tile = left[band, spot]
            chosen.append(jnp.where(use, tile, jnp.zeros_like(tile)))
        term = jnp.dot(
            jnp.concatenate(chosen, axis=0), right[origin, place], preferred_element_type=jnp.float32
        )
        total[...] += term.reshape(total.shape)

    def cube_term(origin, place):
        label = left_labels[origin, 0, place]
        inner = origin * block_cols + lax.rem(label, block_cols)
        band = inner // block_rows
        piece = squares[origin, place]
        for slot, (own_row, own_col, out_row, out_col, live) in enumerate(owns):
            spot, found = find(right_labels, band, lax.rem(inner, block_rows) * block_cols + own_col)
            use = live & found & (label // block_cols == own_row)
            use = use & (mask[out_row, inner] > 0) & (mask[inner, out_col] > 0)
            tile = right[band, spot]
            total[slot] += jnp.dot(
                piece, jnp.where(use, tile, jnp.zeros_like(tile)), preferred_element_type=jnp.float32
            )

    def stack_terms(origin, wait=None):
        for slot in range(slots):
            if wait is not None:
                wait(slot)
            square_term(origin, slot)

    def mate_terms(at):
        stack_terms(2 * at + 1 - lane, lambda slot: from_mate(slot + 1, at).wait_recv())

    def consume(step):
        for way in range(2):
            @pl.when(arrives(way, step))
            def _():
                heading = 1 if way == 0 else -1
                stack_terms(2 * (place - heading * (step + 1)) + lane)
        for way in range(2):
            @pl.when(arrives(way, step))
            def _():
                heading = 1 if way == 0 else -1
                mate_terms(place - heading * (step + 1))

    total[...] = jnp.zeros_like(total)
    turn(0, 0)
    for step in range(1, row_size):
        id_row(step).wait()
    for step in range(1, col_size):
        id_col(step).wait()
    copies = (
        pltpu.make_async_copy(left_ids, left_labels, label_sems.at[0]),
        pltpu.make_async_copy(right_ids, right_labels, label_sems.at[1]),
    )
    for copy in copies:
        copy.start()
    for copy in copies:
        copy.wait()
    left_gather.forward()
    left_gather.collect(None, range(left_gather.chips))
    stack_terms(row)
    mate_terms(place)

    def advance(step, unused):
        turn(step, 0)
        consume(step - 1)
        return unused

    lax.fori_loop(1, length - 1, advance, 0)
    consume(length - 2)

    square[...] = total[...].astype(square.dtype)

    square_gather = ColGather(row, col, col_size, slots, square, squares, square_sems)

    def keep(slot, unused):
        squares[col, slot] = square[slot]
        for step in range(1, square_gather.chips):
            square_gather.across(step, slot).start()
        square_gather.beside(0, slot).start()
        return unused

    lax.fori_loop(0, slots, keep, 0)
    total[...] = jnp.zeros_like(total)
    for slot in range(slots):
        cube_term(col, slot)
    square_gather.collect(cube_term, [0])
    square_gather.forward(cube_term)
    square_gather.collect(cube_term, range(1, square_gather.chips))
    out[...] = (3.0 * square[...].astype(jnp.float32) - 2.0 * total[...]).astype(out.dtype)

    left_gather.settle()
    square_gather.settle()

    def settle(step, unused):
        for index in range(count + 1):
            for way in range(2):
                @pl.when(goes(way, step))
                def _():
                    along(way, step, index).wait_send()
        return unused

    lax.fori_loop(0, length - 1, settle, 0)
    own_to_mate(0).wait_send()

    def collect(at, unused):
        for index in range(1, count):
            to_mate(index, at).wait_send()
        return unused

    lax.fori_loop(0, length, collect, 0)

UNITS = (4, 5)
ROOM = 5
Y_SLOTS = 2
FAR_TERMS = 2
TERMS = 4
PARTS = 4
F32, BF16 = jnp.float32, jnp.bfloat16


def iota(shape, axis):
    return lax.broadcasted_iota(jnp.int32, shape, axis)


def plan_kernel(
    row_size, col_size, slots, far_mask, far_ids, far_tiles, out, choice, tiles, mask, ids, tile_row, tile_col,
    tile_spot, reach, ranges, rows_table, table, across, ahead, behind, stops, sems,
):
    fetches = [
        pltpu.make_async_copy(src, dst, sems.at[number])
        for number, (src, dst) in enumerate(((far_mask, mask), (far_ids, ids), (far_tiles, tiles)))
    ]
    for fetch in fetches:
        fetch.start()
    blocks, lanes = mask.shape[0], 128
    block_rows, block_cols = blocks // row_size, blocks // col_size
    length = row_size // 2
    lines = 4 * col_size
    row, col = lax.axis_index("row"), lax.axis_index("col")
    place, lane = row // 2, lax.rem(row, 2)
    dot = functools.partial(jnp.dot, preferred_element_type=F32)

    fetches[0].wait()
    occupied = mask[...].astype(F32)
    grid = occupied.astype(BF16)
    row_of, lane_of = iota((blocks, lanes), 0), iota((blocks, lanes), 1)
    spread = row_of - lax.rem(lane_of, block_cols)
    keep = lax.rem(row_of, block_rows) == lane_of // block_cols
    before = (iota((lanes, lanes), 0) <= iota((lanes, lanes), 1)).astype(F32).astype(BF16)
    region_of, spot_of = iota((row_size, lanes), 0), iota((row_size, lanes), 1)
    home = spot_of // slots
    tile_home = iota((1, lanes), 1) // slots
    spot_value = (spot_of + 1).astype(F32)
    at = row_of.astype(F32)

    def groups(value):
        return jnp.sum(value.reshape(row_size, block_rows, lanes), axis=1)

    for panel in range(col_size):
        pick = (spread == panel * block_cols).astype(F32).astype(BF16)
        flat = groups(jnp.where(keep, dot(grid, pick), 0.0))
        rank = dot(flat.astype(BF16), before)
        spots = jnp.zeros((row_size, lanes), F32)
        for slot in range(slots):
            found = jnp.where((rank == slot + 1) & (flat > 0), spot_value, 0.0)
            found = jnp.sum(found, axis=1, keepdims=True)
            spots = jnp.where(spot_of == region_of * slots + slot, found, spots)
        spot = jnp.sum(spots, axis=0, keepdims=True) - 1.0
        high = jnp.floor((spot + 0.5) / block_cols)
        block_row = jnp.where(spot >= 0, tile_home.astype(F32) * block_rows + high, -1.0)
        block_col = jnp.where(spot >= 0, panel * block_cols + spot - high * block_cols, -1.0)
        tile_spot[pl.ds(panel, 1), :] = spot
        tile_row[pl.ds(panel, 1), :] = block_row
        tile_col[pl.ds(panel, 1), :] = block_col
        by_row = dot(grid, (at == block_row).astype(F32).astype(BF16))
        by_col = dot(grid, (at == block_col).astype(F32).astype(BF16))
        wanted = (groups(by_row * by_col) > 0) & (region_of != home)
        for side in range(2):
            for way in range(2):
                step = region_of // 2 + 1 if way == 0 else length - region_of // 2
                far = jnp.where(wanted & (lax.rem(region_of, 2) == side), step.astype(F32), 0.0)
                reach[pl.ds((side * 2 + way) * col_size + panel, 1), :] = jnp.max(far, axis=0, keepdims=True)
            gap = jnp.abs(region_of // 2 - home // 2) + 1
            gap = jnp.where(wanted & (lax.rem(region_of, 2) == side), gap.astype(F32), 0.0)
            gap = jnp.max(gap, axis=0, keepdims=True)
            for way in range(2):
                ranges[pl.ds((side * 2 + way) * col_size + panel, 1), :] = gap

    depth = row_size * slots
    far, gaps = reach[...].T[:depth], ranges[...].T[:depth]
    tile, line = iota((depth, lines), 0), iota((depth, lines), 1)
    side, way = line // (2 * col_size), lax.rem(line // col_size, 2)
    origin, number = tile // slots, lax.rem(tile, slots)
    begin = jnp.where(way == 0, origin // 2, length - 1 - origin // 2)
    straight = lax.rem(origin, 2) == side
    crosses = (gaps > 0) & jnp.logical_not(straight)
    number_value = number.astype(F32)
    value = jnp.where(crosses, gaps * 8 - number_value, -8.0)
    order = jnp.zeros((depth, lines), F32)
    for back in range(1, slots):
        order += jnp.where((number >= back) & (pltpu.roll(value, back, 0) > value), 1.0, 0.0)
        order += jnp.where((number + back < slots) & (pltpu.roll(value, depth - back, 0) > value), 1.0, 0.0)
    trouble = jnp.zeros((depth, lines), F32)
    first_ready = jnp.where(straight, 0.0, order + 1)
    first_code = jnp.where(straight, number_value, slots + order)
    weight = far * (128 * 128) - (128 * tile).astype(F32) + 1.0
    stop = jnp.zeros((depth, lines), F32)
    for step in range(length - 1):
        fresh = begin == step
        ready = jnp.where(fresh, first_ready, stop + 1.0)
        key = weight + jnp.where(fresh, first_code, 2 * slots + stop)
        left = jnp.where((far > step + 1) & (begin <= step), 1.0, 0.0)
        for turn in range(ROOM):
            live = jnp.where((left > 0) & (ready <= turn), key, 0.0)
            best = jnp.max(live, axis=0, keepdims=True)
            taken = (live == best) & (live > 0)
            stop = jnp.where(taken, float(turn), stop)
            left = jnp.where(taken, 0.0, left)
            rows_table[pl.ds(step * 8 + turn, 1), :] = best
            if turn + 1 in UNITS:
                trouble = jnp.maximum(trouble, left * (UNITS.index(turn + 1) + 1.0))
        stops[step] = stop
    codes = rows_table[...]
    codes = jnp.maximum(codes - 128 * jnp.floor(codes / 128) - 1.0, 0.0)
    table[:, : codes.shape[0]] = codes.T
    across[:, :depth] = jnp.where(crosses, order + 1.0, 0.0).T
    ahead[:, :depth] = stops[jnp.maximum(place - 1, 0)].T
    behind[:, :depth] = stops[jnp.maximum(length - 2 - place, 0)].T

    here, there = (lane * 2) * col_size + col, (lane * 2 + 1) * col_size + col
    other = (1 - lane) * 2 * col_size + col
    tile, tile_number = iota((1, lanes), 1), lax.rem(iota((1, lanes), 1), slots)
    tile_place = tile_home // 2
    my_rows, my_cols = tile_row[pl.ds(col, 1), :], tile_col[pl.ds(col, 1), :]
    beyond, under = ahead[pl.ds(here, 1), :], behind[pl.ds(there, 1), :]
    spot = jnp.where(tile_place < place, 2 * slots + beyond, 2 * slots + ROOM + under)
    spot = jnp.where(tile_place == place, slots - 1 + across[pl.ds(here, 1), :], spot)
    spot = jnp.where(tile_home == row, tile_number.astype(F32), spot)

    inside = iota((blocks, blocks), 0), iota((blocks, blocks), 1)
    same_rows = inside[0] // block_rows == inside[1] // block_rows
    same_cols = inside[0] // block_cols == inside[1] // block_cols
    lower = (same_rows & (inside[1] < inside[0])).astype(F32).astype(BF16)
    whole = same_cols.astype(F32).astype(BF16)
    upper = (same_cols & (inside[0] < inside[1])).astype(F32).astype(BF16)
    chip_of = inside[1] // (2 * block_cols)
    flipped = occupied.T.astype(BF16)
    shared = dot(grid, flipped)
    inner = near_count = jnp.zeros((blocks, blocks), F32)
    for chip in range(col_size // 2):
        on_chip = jnp.where(chip_of == chip, occupied, 0.0).astype(BF16)
        inner = jnp.where(chip_of == chip, dot(on_chip, flipped), inner)
        near_count = jnp.where(chip_of == chip, dot(on_chip, grid), near_count)
    leaves = jnp.where((occupied > 0) & (shared > inner), 1.0, 0.0)
    gone = leaves.astype(BF16)
    ranks = dot(dot(lower, grid).astype(BF16), whole) + dot(grid, upper)
    y_ranks = dot(dot(lower, gone).astype(BF16), whole) + dot(gone, upper)
    panels = ((inside[1] // block_cols) * slots).astype(F32)
    labels = ranks + panels
    y_labels = jnp.where(chip_of == col // 2, ranks, y_ranks) + panels
    y_order = leaves * (y_ranks + 1.0)

    def peak(value):
        return jnp.max(jnp.max(value, axis=1, keepdims=True), axis=0, keepdims=True)

    joint = dot(grid, grid)
    fan = peak(joint * occupied)
    crowd = jnp.maximum(peak(y_order) - Y_SLOTS, peak((joint - near_count) * occupied) - FAR_TERMS)

    chosen = (at == my_rows).astype(F32).astype(BF16)
    met = dot(grid, chosen)
    named, y_named = dot(labels.astype(BF16), chosen), dot(y_labels.astype(BF16), chosen)
    sub, column = iota((8, lanes), 0), iota((8, lanes), 1)
    deep, wide = iota((16, lanes), 0), iota((16, lanes), 1)
    pairs = jnp.zeros((16, lanes), F32)
    near = jnp.floor((my_rows + 0.5) / (2 * block_cols)) == (col // 2).astype(F32)
    result = jnp.where(sub == 0, table[pl.ds(here, 1), :], 0.0)
    result = jnp.where(sub == 1, table[pl.ds(there, 1), :], result)
    inside_rows, inside_cols = inside[0].astype(F32), inside[1].astype(F32)
    for slot in range(slots):
        mine = tile == row * slots + slot
        out_row = jnp.sum(jnp.where(mine, my_rows, 0.0), axis=1, keepdims=True)
        out_col = jnp.sum(jnp.where(mine, my_cols, 0.0), axis=1, keepdims=True)
        on_row = at == out_row
        joins = jnp.sum(jnp.where(on_row, met, 0.0), axis=0, keepdims=True)
        name = jnp.sum(jnp.where(on_row, named, 0.0), axis=0, keepdims=True)
        y_name = jnp.sum(jnp.where(on_row, y_named, 0.0), axis=0, keepdims=True)
        use = (joins > 0) & (my_cols == out_col) & (my_rows >= 0)
        pairs = jnp.where((deep == slot) & use, name * 64 + spot + 1, pairs)
        pairs = jnp.where((deep == slot + slots) & use & near, y_name * 64 + spot + 1, pairs)
        pairs = jnp.where((deep == slot + 2 * slots) & use & jnp.logical_not(near), y_name * 64 + spot + 1, pairs)
        y_spot = jnp.where((inside_rows == out_row) & (inside_cols == out_col), y_order, 0.0)
        y_spot = jnp.sum(jnp.sum(y_spot, axis=1, keepdims=True), axis=0, keepdims=True)
        result = jnp.where((sub == 6) & (column == 8 + slot), y_spot, result)
    product = jnp.zeros((16, lanes), F32)
    shifted = wide - 16 * (deep // slots)
    for term in range(TERMS):
        best = jnp.max(pairs, axis=1, keepdims=True)
        pairs = jnp.where(pairs == best, 0.0, pairs)
        product = jnp.where(shifted == term, best, product)

    fetches[1].wait()
    level = peak(trouble)
    kind = 2.0 * level + jnp.where((crowd > 0) & (level < 2), 1.0, 0.0)
    choice[...] = jnp.where(fan > TERMS, 4.0, kind).astype(jnp.int32)
    for slot in range(slots):
        mine = tile == row * slots + slot
        label = ids[0:1, slot : slot + 1].astype(F32)
        owner = (tile_home == row) & (tile_spot[pl.ds(col, 1), :] == label)
        name = jnp.sum(jnp.where(owner, tile_number.astype(F32) + 1.0, 0.0), axis=1, keepdims=True)
        order = jnp.where(mine, across[pl.ds(other, 1), :], 0.0)
        order = jnp.sum(order, axis=1, keepdims=True)
        result = jnp.where((sub == 6) & (column == slot), name, result)
        result = jnp.where((sub == 2) & (column == slot), order, result)
        every = jnp.where(lax.rem(deep, slots) == slot, product, 0.0)
        result = jnp.where(sub == 3 + slot, jnp.sum(every, axis=0, keepdims=True), result)
    out[...] = result.astype(jnp.int32)
    fetches[2].wait()


def make_plan(mesh, mask, ids, stack):
    row_size, col_size = mesh.shape["row"], mesh.shape["col"]
    slots, steps = stack.shape[0], row_size // 2 - 1
    panel, lines = pltpu.VMEM((col_size, 128), F32), 4 * col_size
    wide = pltpu.VMEM((lines, 128), F32)
    return pl.pallas_call(
        functools.partial(plan_kernel, row_size, col_size, slots),
        out_shape=(
            jax.ShapeDtypeStruct((8, 128), jnp.int32),
            jax.ShapeDtypeStruct((1, 1), jnp.int32),
            jax.ShapeDtypeStruct(stack.shape, stack.dtype),
        ),
        in_specs=[HBM, HBM, HBM],
        out_specs=(VMEM, VMEM, VMEM),
        scratch_shapes=[
            pltpu.VMEM(mask.shape, mask.dtype), pltpu.VMEM(ids.shape, ids.dtype), panel, panel, panel, wide, wide,
            pltpu.VMEM((8 * steps, lines), F32), wide, wide, wide, wide,
            pltpu.VMEM((steps, row_size * slots, lines), F32), pltpu.SemaphoreType.DMA((3,)),
        ],
        compiler_params=pltpu.CompilerParams(vmem_limit_bytes=16 * 2**20),
        name="plan",
    )(mask, ids, stack)


def sparse_kernel(
    row_size, col_size, units, y_slots, far_terms, plan, tiles, out, canon, x_out, left, held, squares, near, square,
    total, final, y_out, z_out, col_sems, square_sems, x_sems, z_sems,
):
    row, col = lax.axis_index("row"), lax.axis_index("col")
    slots, side = canon.shape[0], canon.shape[1]
    rows = side // PARTS
    length = row_size // 2
    place, lane = row // 2, lax.rem(row, 2)
    mate = row + 1 - 2 * lane
    chips = col_size // 2
    chip, core = col // 2, lax.rem(col, 2)
    x_units = slots

    barrier = pltpu.get_barrier_semaphore()

    def hello(to_row, to_col):
        pl.semaphore_signal(barrier, inc=1, device_id=(to_row, to_col), device_id_type=MESH)

    hello(mate, col)
    hello(row, col + 1 - 2 * core)
    for step in range(1, chips):
        hello(row, 2 * lax.rem(chip + step, chips) + core)
    for way in range(2):
        @pl.when((place + 1 < length) if way == 0 else (place > 0))
        def _():
            hello(row + 2 - 4 * way, col)

    for number in range(slots):
        tile = jnp.zeros((side, side), tiles.dtype)
        for slot in range(slots):
            tile = jnp.where(plan[6, slot] == number + 1, tiles[slot], tile)
        canon[number] = tile
    for slot in range(slots):
        tile = canon[0]
        for number in range(1, slots):
            tile = jnp.where(plan[2, number] == slot + 1, canon[number], tile)
        x_out[slot] = tile

    ends = jnp.where(place == 0, 1, 0) + jnp.where(place + 1 == length, 1, 0)
    pl.semaphore_wait(barrier, 2 + chips - 1 + 2 - ends)

    def x_copy(unit, part):
        span = pl.ds(part * rows, rows)
        return send(
            x_out.at[unit, span], held.at[slots + unit, span],
            x_sems.at[0, unit, part], x_sems.at[1, unit, part], mate, col,
        )

    def z_copy(way, unit, part):
        span = pl.ds(part * rows, rows)
        return send(
            z_out.at[way, unit, span], held.at[2 * slots + way * ROOM + unit, span],
            z_sems.at[way, 0, unit, part], z_sems.at[way, 1, unit, part], row + 2 - 4 * way, col,
        )

    for unit in range(x_units):
        for part in range(PARTS):
            x_copy(unit, part).start()
    left_gather = ColGather(row, col, col_size, slots, canon, left, col_sems)
    left_gather.start()

    done = (place, length - 1 - place)
    for unit in range(units):
        for way in range(2):
            @pl.when(done[way] + 1 < length)
            def _():
                code = plan[way, done[way] * 8 + unit]
                piece = canon[0]
                for other in range(1, slots):
                    piece = jnp.where(code == other, canon[other], piece)
                for other in range(min(unit - 1, x_units)):
                    piece = jnp.where(code == slots + other, held[slots + other], piece)
                for other in range(unit - 1):
                    piece = jnp.where(code == 2 * slots + other, held[2 * slots + way * ROOM + other], piece)
                z_out[way, unit] = piece

        for part in range(PARTS):
            span = pl.ds(part * rows, rows)
            if 1 <= unit <= x_units:
                x_copy(unit - 1, part).wait_recv()
            for way in range(2):
                @pl.when(done[way] + 1 < length)
                def _():
                    if unit:
                        @pl.when(done[way] > 0)
                        def _():
                            z_copy(way, unit - 1, part).wait_recv()

                        code = plan[way, done[way] * 8 + unit]
                        piece = z_out[way, unit, span]
                        if unit <= x_units:
                            spot = slots + unit - 1
                            piece = jnp.where(code == spot, held[spot, span], piece)
                        spot = 2 * slots + unit - 1
                        piece = jnp.where(code == spot, held[spot + way * ROOM, span], piece)
                        z_out[way, unit, span] = piece
                    z_copy(way, unit, part).start()

    left_gather.forward()
    for number in range(slots):
        held[number] = canon[number]
        left[col, number] = canon[number]

    for unit in range(units - 1, x_units):
        for part in range(PARTS):
            x_copy(unit, part).wait_recv()
    for way in range(2):
        @pl.when(done[way] + 1 == length)
        def _():
            for unit in range(units - 1):
                for part in range(PARTS):
                    z_copy(way, unit, part).wait_recv()

        @pl.when(done[way] > 0)
        def _():
            for part in range(PARTS):
                z_copy(way, units - 1, part).wait_recv()

    left_gather.collect(None, range(left_gather.chips))

    def sum_terms(panel, number, first, terms):
        result = jnp.zeros((side, side), F32)
        for term in range(terms):
            code = plan[3 + number, first + term]
            pair = jnp.maximum(code - 1, 0)
            name, spot = pair // 64, lax.rem(pair, 64)
            tile = panel[lax.rem(name // slots, panel.shape[0]), lax.rem(name, slots)]
            result += jnp.dot(
                jnp.where(code > 0, tile, jnp.zeros_like(tile)), held[spot], preferred_element_type=F32,
            )
        return result

    square_gather = ColGather(row, col, col_size, slots, square, squares, square_sems, y_out, y_slots, near)

    for slot in range(y_slots):
        number = jnp.int32(0)
        for other in range(1, slots):
            number = jnp.where(plan[6, 8 + other] == slot + 1, other, number)
        y_out[slot] = sum_terms(left, number, 0, TERMS).astype(square.dtype)
        for step in range(1, chips):
            square_gather.across(step, slot).start()

    def first(number, unused):
        tile = sum_terms(left, number, 0, TERMS).astype(square.dtype)
        square[number] = tile
        near[core, number] = tile
        square_gather.beside(0, number).start()
        return unused

    lax.fori_loop(0, slots, first, 0)
    square_gather.collect(None, [0])

    def second(number, unused):
        total[number] = sum_terms(near, number, 16, TERMS)
        return unused

    lax.fori_loop(0, slots, second, 0)
    square_gather.forward()
    square_gather.collect(None, range(1, chips))

    def third(number, unused):
        cube = total[number] + sum_terms(squares, number, 32, far_terms)
        final[number] = (3.0 * square[number].astype(F32) - 2.0 * cube).astype(final.dtype)
        return unused

    lax.fori_loop(0, slots, third, 0)
    for slot in range(slots):
        tile = jnp.zeros((side, side), out.dtype)
        for number in range(slots):
            tile = jnp.where(plan[6, slot] == number + 1, final[number], tile)
        out[slot] = tile

    left_gather.settle()
    square_gather.settle()

    for part in range(PARTS):
        for unit in range(x_units):
            x_copy(unit, part).wait_send()
    for way in range(2):
        @pl.when(done[way] + 1 < length)
        def _():
            for unit in range(units):
                for part in range(PARTS):
                    z_copy(way, unit, part).wait_send()


def room(panels, slots, side):
    return (4 * panels + 16) * slots * side * side * 2 + 8 * 2**20


def sparse_step(mesh, units, y_slots, far_terms, barrier_id, plan, stack):
    row_size, col_size = mesh.shape["row"], mesh.shape["col"]
    chips = col_size // 2
    slots, side, _ = stack.shape
    dma = pltpu.SemaphoreType.DMA

    def tiles(*count):
        return pltpu.VMEM((*count, side, side), stack.dtype)

    return pl.pallas_call(
        functools.partial(sparse_kernel, row_size, col_size, units, y_slots, far_terms),
        out_shape=jax.ShapeDtypeStruct(stack.shape, stack.dtype),
        in_specs=[SMEM, VMEM],
        out_specs=VMEM,
        scratch_shapes=[
            tiles(slots), tiles(slots), tiles(col_size, slots), tiles(2 * slots + 2 * ROOM), tiles(col_size, slots),
            tiles(2, slots), tiles(slots), pltpu.VMEM(stack.shape, F32), tiles(slots), tiles(y_slots), tiles(2, units),
            dma((4, chips, slots)), dma((4, chips, slots)), dma((2, slots, PARTS)), dma((2, 2, units, PARTS)),
        ],
        compiler_params=pltpu.CompilerParams(
            collective_id=barrier_id, has_side_effects=True, vmem_limit_bytes=room(col_size, slots, side)
        ),
        name="sparse",
    )(plan, stack)


def dense_step(mesh, ids, stack, mask):
    row_size, col_size = mesh.shape["row"], mesh.shape["col"]
    length, chips = row_size // 2, col_size // 2
    dma = pltpu.SemaphoreType.DMA
    slots, side, _ = stack.shape
    col_panel = pltpu.VMEM((col_size, slots, side, side), stack.dtype)
    return pl.pallas_call(
        functools.partial(dense_kernel, row_size, col_size),
        out_shape=jax.ShapeDtypeStruct(stack.shape, stack.dtype),
        in_specs=[VMEM, SMEM, SMEM],
        out_specs=VMEM,
        scratch_shapes=[
            col_panel,
            pltpu.VMEM((row_size, slots, side, side), stack.dtype),
            col_panel,
            pltpu.VMEM(stack.shape, stack.dtype),
            pltpu.VMEM(stack.shape, jnp.float32),
            pltpu.VMEM((col_size, 8, 128), jnp.int32),
            pltpu.VMEM((row_size, 8, 128), jnp.int32),
            pltpu.VMEM((8, 128), jnp.int32),
            pltpu.SMEM((col_size, 8, 128), jnp.int32),
            pltpu.SMEM((row_size, 8, 128), jnp.int32),
            dma((4, chips, slots)),
            dma((4, chips, slots)),
            dma((2, 2, length, slots + 2)),
            dma((2, length, slots + 1)),
            dma((2, row_size)),
            dma((2, col_size)),
            dma((2,)),
        ],
        compiler_params=pltpu.CompilerParams(
            collective_id=0, has_side_effects=True, vmem_limit_bytes=room(row_size + col_size, slots, side)
        ),
        name="purify",
    )(stack, ids, mask)


def solution(mesh):
    def local(tiles, stack_index, block_mask):
        stack = tiles[0, 0]
        plan, choice, fetched = make_plan(mesh, block_mask, stack_index[0], stack)
        slots = stack.shape[0]
        sizes = (
            (UNITS[0], Y_SLOTS, FAR_TERMS), (UNITS[0], slots, TERMS),
            (UNITS[1], Y_SLOTS, FAR_TERMS), (UNITS[1], slots, TERMS),
        )
        branches = [
            functools.partial(sparse_step, mesh, *size, number + 1, plan, fetched) for number, size in enumerate(sizes)
        ]
        branches = [lambda branch=branch: branch() for branch in branches]
        branches.append(lambda: dense_step(mesh, stack_index[0], stack, block_mask))
        purified = _switch_internal(choice[0, 0], branches, (), branches_platforms=None)
        return purified[None, None]

    placed = (P("row", "col", None, None, None), P("row", "col", None), P())
    return jax.shard_map(
        local,
        mesh=mesh,
        in_specs=placed,
        out_specs=P("row", "col", None, None, None),
        check_vma=False,
    )
```

```python
import functools

import jax
import jax.numpy as jnp
from jax import lax
from jax.experimental import pallas as pl
from jax.experimental.pallas import tpu as pltpu
from jax.sharding import PartitionSpec as P
from jax._src.lax.control_flow.conditionals import _switch_internal

MESH = pl.DeviceIdType.MESH
VMEM = pl.BlockSpec(memory_space=pltpu.VMEM)
SMEM = pl.BlockSpec(memory_space=pltpu.SMEM)
HBM = pl.BlockSpec(memory_space=pltpu.HBM)


def send(src, dst, send_sem, recv_sem, row, col):
    return pltpu.make_async_remote_copy(
        src_ref=src,
        dst_ref=dst,
        send_sem=send_sem,
        recv_sem=recv_sem,
        device_id=(row, col),
        device_id_type=MESH,
    )


def greet(row_size, col_size, row, col, with_rows):
    barrier = pltpu.get_barrier_semaphore()
    count = col_size - 1
    for step in range(1, col_size):
        peer = lax.rem(col + step, col_size)
        pl.semaphore_signal(barrier, inc=1, device_id=(row, peer), device_id_type=MESH)
    if with_rows:
        count += row_size - 1
        for step in range(1, row_size):
            peer = lax.rem(row + step, row_size)
            pl.semaphore_signal(barrier, inc=1, device_id=(peer, col), device_id_type=MESH)
    pl.semaphore_wait(barrier, count)


class ColGather:
    def __init__(self, row, col, col_size, slots, own, panel, sems, far=None, far_slots=None, near=None):
        self.row, self.col, self.slots = row, col, slots
        self.own, self.panel, self.sems = own, panel, sems
        self.far, self.near = own if far is None else far, near
        self.far_slots = slots if far_slots is None else far_slots
        self.chips = col_size // 2
        self.chip, self.core = col // 2, lax.rem(col, 2)
        self.partner = col + 1 - 2 * self.core

    def across(self, step, slot):
        target = 2 * lax.rem(self.chip + step, self.chips) + self.core
        return send(
            self.far.at[slot], self.panel.at[self.col, slot],
            self.sems.at[0, step - 1, slot], self.sems.at[1, step - 1, slot], self.row, target,
        )

    def beside(self, step, slot):
        origin = 2 * lax.rem(self.chip + self.chips - step, self.chips) + self.core
        src = self.own.at[slot] if step == 0 else self.panel.at[origin, slot]
        near = self.near is not None and step == 0
        return send(
            src, self.near.at[self.core, slot] if near else self.panel.at[origin, slot],
            self.sems.at[2, step, slot], self.sems.at[3, step, slot], self.row, self.partner,
        )

    def start(self):
        for slot in range(self.slots):
            for step in range(1, self.chips):
                self.across(step, slot).start()
        for slot in range(self.slots):
            self.beside(0, slot).start()

    def origin(self, step, core):
        return 2 * lax.rem(self.chip + self.chips - step, self.chips) + core

    def forward(self, use=None):
        for slot in range(self.far_slots):
            for step in range(1, self.chips):
                self.across(step, slot).wait_recv()
                self.beside(step, slot).start()
                if use is not None:
                    use(self.origin(step, self.core), slot)

    def count(self, step):
        return self.far_slots if step else self.slots

    def collect(self, use, steps):
        for step in steps:
            for slot in range(self.count(step)):
                self.beside(step, slot).wait_recv()
                if use is not None:
                    use(self.origin(step, 1 - self.core), slot)

    def settle(self):
        for step in range(self.chips):
            for slot in range(self.count(step)):
                if step:
                    self.across(step, slot).wait_send()
                self.beside(step, slot).wait_send()


def dense_kernel(
    row_size, col_size, tiles, ids, mask, out, left, right, squares, square, total, left_ids, right_ids, ids_out,
    left_labels, right_labels, col_sems, square_sems, line_sems, side_sems, row_id_sems, col_id_sems, label_sems,
):
    row, col = lax.axis_index("row"), lax.axis_index("col")
    slots, side = tiles.shape[0], tiles.shape[1]
    half = side // 2
    length = row_size // 2
    place, lane = row // 2, lax.rem(row, 2)
    mate = row + 1 - 2 * lane

    lane_iota = lax.broadcasted_iota(jnp.int32, (8, 128), 1)
    packed = jnp.full((8, 128), -1, jnp.int32)
    for slot in range(slots):
        packed = jnp.where(lane_iota == slot, ids[0, slot], packed)
    ids_out[...] = packed
    greet(row_size, col_size, row, col, True)

    pieces = [(slot, 0, side, False) for slot in range(slots - 1)]
    cut = side * 64 // 256
    pieces += [(slots - 1, cut, side - cut, False)]
    early = (slots - 1, 0, cut, True)
    mine = [early] + pieces
    count = len(mine)

    def view(ref, piece, origin=None):
        slot, first, rows, _ = piece
        if origin is None:
            return ref.at[slot, pl.ds(first, rows)]
        return ref.at[origin, slot, pl.ds(first, rows)]

    def to_mate(index, at):
        piece = mine[index]
        origin = 2 * at + lane
        return send(
            view(right, piece, origin), view(right, piece, origin),
            side_sems.at[0, at, index], side_sems.at[1, at, index], mate, col,
        )

    def own_to_mate(index):
        piece = mine[index]
        return send(
            view(tiles, piece), view(right, piece, row),
            side_sems.at[0, place, index], side_sems.at[1, place, index], mate, col,
        )

    def from_mate(index, at):
        piece = mine[index]
        origin = 2 * at + 1 - lane
        return send(
            view(right, piece, origin), view(right, piece, origin),
            side_sems.at[0, at, index], side_sems.at[1, at, index], mate, col,
        )

    def along(way, step, index, first=False):
        heading = 1 if way == 0 else -1
        piece = mine[0] if index == count else mine[index]
        on_lane = 1 - lane if index == count else lane
        origin = 2 * (place - heading * step) + on_lane
        src = view(tiles, piece) if first and index < count else view(right, piece, origin)
        return send(
            src, view(right, piece, origin),
            line_sems.at[way, 0, step, index], line_sems.at[way, 1, step, index],
            row + 2 * heading, col,
        )

    def landing(way, step, index):
        heading = 1 if way == 0 else -1
        piece = mine[0] if index == count else mine[index]
        on_lane = 1 - lane if index == count else lane
        origin = 2 * (place - heading * (step + 1)) + on_lane
        return send(
            view(right, piece, origin), view(right, piece, origin),
            line_sems.at[way, 0, step, index], line_sems.at[way, 1, step, index],
            row + 2 * heading, col,
        )

    can_send = (place + 1 < length, place > 0)

    def arrives(way, step):
        return place - step >= 1 if way == 0 else place + step + 1 < length

    def goes(way, step):
        if way == 0:
            return (place - step >= 0) & (place + 1 < length)
        return (place + step < length) & (place > 0)

    def id_row(step):
        return send(
            ids_out, right_ids.at[row], row_id_sems.at[0, step], row_id_sems.at[1, step],
            lax.rem(row + step, row_size), col,
        )

    def id_col(step):
        return send(
            ids_out, left_ids.at[col], col_id_sems.at[0, step], col_id_sems.at[1, step],
            row, lax.rem(col + step, col_size),
        )

    for step in range(1, row_size):
        id_row(step).start()
    for step in range(1, col_size):
        id_col(step).start()

    left_gather = ColGather(row, col, col_size, slots, tiles, left, col_sems)
    left_gather.start()
    own_to_mate(0).start()
    for index in range(count):
        for way in range(2):
            @pl.when(can_send[way])
            def _():
                along(way, 0, index, True).start()
        if index:
            own_to_mate(index).start()


    from_mate(0, place).wait_recv()
    for way in range(2):
        @pl.when(can_send[way])
        def _():
            along(way, 0, count).start()

    right[row] = tiles[...]
    left[col] = tiles[...]
    right_ids[row] = packed
    left_ids[col] = packed

    def turn(step, unused):
        for index in list(range(count)) + [count]:
            for way in range(2):
                @pl.when(arrives(way, step))
                def _():
                    landing(way, step, index).wait_recv()

                    @pl.when(can_send[way])
                    def _():
                        along(way, step + 1, index).start()

                    if 0 < index < count:
                        heading = 1 if way == 0 else -1
                        to_mate(index, place - heading * (step + 1)).start()
        return unused

    block_rows, block_cols = mask.shape[0] // row_size, mask.shape[1] // col_size
    owns = []
    for slot in range(slots):
        own = ids[0, slot]
        own_row, own_col = own // block_cols, lax.rem(own, block_cols)
        out_row, out_col = row * block_rows + own_row, col * block_cols + own_col
        owns.append((own_row, own_col, out_row, out_col, mask[out_row, out_col] > 0))

    def find(labels, region, wanted):
        spot, found = jnp.int32(0), labels[region, 0, 0] == wanted
        for other in range(1, slots):
            same = labels[region, 0, other] == wanted
            spot = jnp.where(same, other, spot)
            found = found | same
        return spot, found

    def square_term(origin, place):
        label = right_labels[origin, 0, place]
        inner = origin * block_rows + label // block_cols
        band = inner // block_cols
        chosen = []
        for own_row, own_col, out_row, out_col, live in owns:
            spot, found = find(left_labels, band, own_row * block_cols + lax.rem(inner, block_cols))
            use = live & found & (lax.rem(label, block_cols) == own_col)
            use = use & (mask[out_row, inner] > 0) & (mask[inner, out_col] > 0)
            tile = left[band, spot]
            chosen.append(jnp.where(use, tile, jnp.zeros_like(tile)))
        term = jnp.dot(
            jnp.concatenate(chosen, axis=0), right[origin, place], preferred_element_type=jnp.float32
        )
        total[...] += term.reshape(total.shape)

    def cube_term(origin, place):
        label = left_labels[origin, 0, place]
        inner = origin * block_cols + lax.rem(label, block_cols)
        band = inner // block_rows
        piece = squares[origin, place]
        for slot, (own_row, own_col, out_row, out_col, live) in enumerate(owns):
            spot, found = find(right_labels, band, lax.rem(inner, block_rows) * block_cols + own_col)
            use = live & found & (label // block_cols == own_row)
            use = use & (mask[out_row, inner] > 0) & (mask[inner, out_col] > 0)
            tile = right[band, spot]
            total[slot] += jnp.dot(
                piece, jnp.where(use, tile, jnp.zeros_like(tile)), preferred_element_type=jnp.float32
            )

    def stack_terms(origin, wait=None):
        for slot in range(slots):
            if wait is not None:
                wait(slot)
            square_term(origin, slot)

    def mate_terms(at):
        stack_terms(2 * at + 1 - lane, lambda slot: from_mate(slot + 1, at).wait_recv())

    def consume(step):
        for way in range(2):
            @pl.when(arrives(way, step))
            def _():
                heading = 1 if way == 0 else -1
                stack_terms(2 * (place - heading * (step + 1)) + lane)
        for way in range(2):
            @pl.when(arrives(way, step))
            def _():
                heading = 1 if way == 0 else -1
                mate_terms(place - heading * (step + 1))

    total[...] = jnp.zeros_like(total)
    turn(0, 0)
    for step in range(1, row_size):
        id_row(step).wait()
    for step in range(1, col_size):
        id_col(step).wait()
    copies = (
        pltpu.make_async_copy(left_ids, left_labels, label_sems.at[0]),
        pltpu.make_async_copy(right_ids, right_labels, label_sems.at[1]),
    )
    for copy in copies:
        copy.start()
    for copy in copies:
        copy.wait()
    left_gather.forward()
    left_gather.collect(None, range(left_gather.chips))
    stack_terms(row)
    mate_terms(place)

    def advance(step, unused):
        turn(step, 0)
        consume(step - 1)
        return unused

    lax.fori_loop(1, length - 1, advance, 0)
    consume(length - 2)

    square[...] = total[...].astype(square.dtype)

    square_gather = ColGather(row, col, col_size, slots, square, squares, square_sems)

    def keep(slot, unused):
        squares[col, slot] = square[slot]
        for step in range(1, square_gather.chips):
            square_gather.across(step, slot).start()
        square_gather.beside(0, slot).start()
        return unused

    lax.fori_loop(0, slots, keep, 0)
    total[...] = jnp.zeros_like(total)
    for slot in range(slots):
        cube_term(col, slot)
    square_gather.collect(cube_term, [0])
    square_gather.forward(cube_term)
    square_gather.collect(cube_term, range(1, square_gather.chips))
    out[...] = (3.0 * square[...].astype(jnp.float32) - 2.0 * total[...]).astype(out.dtype)

    left_gather.settle()
    square_gather.settle()

    def settle(step, unused):
        for index in range(count + 1):
            for way in range(2):
                @pl.when(goes(way, step))
                def _():
                    along(way, step, index).wait_send()
        return unused

    lax.fori_loop(0, length - 1, settle, 0)
    own_to_mate(0).wait_send()

    def collect(at, unused):
        for index in range(1, count):
            to_mate(index, at).wait_send()
        return unused

    lax.fori_loop(0, length, collect, 0)

UNITS = (4, 5)
ROOM = 5
Y_SLOTS = 2
FAR_TERMS = 2
TERMS = 4
PARTS = 4
F32, BF16 = jnp.float32, jnp.bfloat16


def iota(shape, axis):
    return lax.broadcasted_iota(jnp.int32, shape, axis)


def plan_kernel(
    row_size, col_size, slots, far_mask, far_ids, far_tiles, out, choice, tiles, mask, ids, tile_row, tile_col,
    tile_spot, reach, ranges, rows_table, table, across, ahead, behind, stops, sems,
):
    fetches = [
        pltpu.make_async_copy(src, dst, sems.at[number])
        for number, (src, dst) in enumerate(((far_mask, mask), (far_ids, ids), (far_tiles, tiles)))
    ]
    for fetch in fetches:
        fetch.start()
    blocks, lanes = mask.shape[0], 128
    block_rows, block_cols = blocks // row_size, blocks // col_size
    length = row_size // 2
    lines = 4 * col_size
    row, col = lax.axis_index("row"), lax.axis_index("col")
    place, lane = row // 2, lax.rem(row, 2)
    dot = functools.partial(jnp.dot, preferred_element_type=F32)

    fetches[0].wait()
    occupied = mask[...].astype(F32)
    grid = occupied.astype(BF16)
    row_of, lane_of = iota((blocks, lanes), 0), iota((blocks, lanes), 1)
    spread = row_of - lax.rem(lane_of, block_cols)
    keep = lax.rem(row_of, block_rows) == lane_of // block_cols
    before = (iota((lanes, lanes), 0) <= iota((lanes, lanes), 1)).astype(F32).astype(BF16)
    region_of, spot_of = iota((row_size, lanes), 0), iota((row_size, lanes), 1)
    home = spot_of // slots
    tile_home = iota((1, lanes), 1) // slots
    at = row_of.astype(F32)

    def groups(value):
        return jnp.sum(value.reshape(row_size, block_rows, lanes), axis=1)

    flat = []
    for panel in range(col_size):
        pick = (spread == panel * block_cols).astype(F32).astype(BF16)
        flat.append(groups(jnp.where(keep, dot(grid, pick), 0.0)))
    flat = jnp.concatenate(flat, axis=0)
    every = iota(flat.shape, 0), iota(flat.shape, 1)
    first_lane, every_value = lax.rem(every[0], row_size) * slots, (every[1] + 1).astype(F32)
    rank = dot(flat.astype(BF16), before)
    spots = jnp.zeros(flat.shape, F32)
    for slot in range(slots):
        found = jnp.where((rank == slot + 1) & (flat > 0), every_value, 0.0)
        found = jnp.sum(found, axis=1, keepdims=True)
        spots = jnp.where(every[1] == first_lane + slot, found, spots)
    spot = jnp.sum(spots.reshape(col_size, row_size, lanes), axis=1) - 1.0
    high = jnp.floor((spot + 0.5) / block_cols)
    base_row = ((iota((col_size, lanes), 1) // slots) * block_rows).astype(F32)
    base_col = (iota((col_size, lanes), 0) * block_cols).astype(F32)
    block_row = jnp.where(spot >= 0, base_row + high, -1.0)
    block_col = jnp.where(spot >= 0, base_col + spot - high * block_cols, -1.0)
    tile_spot[...], tile_row[...], tile_col[...] = spot, block_row, block_col
    by_rows = [
        dot(grid, (at == block_row[panel : panel + 1]).astype(F32).astype(BF16)) for panel in range(col_size)
    ]
    by_cols = [
        dot(grid, (at == block_col[panel : panel + 1]).astype(F32).astype(BF16)) for panel in range(col_size)
    ]
    for panel, (by_row, by_col) in enumerate(zip(by_rows, by_cols)):
        wanted = (groups(by_row * by_col) > 0) & (region_of != home)
        for side in range(2):
            for way in range(2):
                step = region_of // 2 + 1 if way == 0 else length - region_of // 2
                far = jnp.where(wanted & (lax.rem(region_of, 2) == side), step.astype(F32), 0.0)
                reach[pl.ds((side * 2 + way) * col_size + panel, 1), :] = jnp.max(far, axis=0, keepdims=True)
            gap = jnp.abs(region_of // 2 - home // 2) + 1
            gap = jnp.where(wanted & (lax.rem(region_of, 2) == side), gap.astype(F32), 0.0)
            gap = jnp.max(gap, axis=0, keepdims=True)
            for way in range(2):
                ranges[pl.ds((side * 2 + way) * col_size + panel, 1), :] = gap

    depth = row_size * slots
    far, gaps = reach[...].T[:depth], ranges[...].T[:depth]
    tile, line = iota((depth, lines), 0), iota((depth, lines), 1)
    side, way = line // (2 * col_size), lax.rem(line // col_size, 2)
    origin, number = tile // slots, lax.rem(tile, slots)
    begin = jnp.where(way == 0, origin // 2, length - 1 - origin // 2)
    straight = lax.rem(origin, 2) == side
    crosses = (gaps > 0) & jnp.logical_not(straight)
    number_value = number.astype(F32)
    value = jnp.where(crosses, gaps * 8 - number_value, -8.0)
    order = jnp.zeros((depth, lines), F32)
    for back in range(1, slots):
        order += jnp.where((number >= back) & (pltpu.roll(value, back, 0) > value), 1.0, 0.0)
        order += jnp.where((number + back < slots) & (pltpu.roll(value, depth - back, 0) > value), 1.0, 0.0)
    trouble = jnp.zeros((depth, lines), F32)
    first_ready = jnp.where(straight, 0.0, order + 1)
    first_code = jnp.where(straight, number_value, slots + order)
    weight = far * (128 * 128) - (128 * tile).astype(F32) + 1.0
    stop = jnp.zeros((depth, lines), F32)
    for step in range(length - 1):
        fresh = begin == step
        ready = jnp.where(fresh, first_ready, stop + 1.0)
        key = weight + jnp.where(fresh, first_code, 2 * slots + stop)
        left = jnp.where((far > step + 1) & (begin <= step), 1.0, 0.0)
        for turn in range(ROOM):
            live = jnp.where((left > 0) & (ready <= turn), key, 0.0)
            best = jnp.max(live, axis=0, keepdims=True)
            taken = (live == best) & (live > 0)
            stop = jnp.where(taken, float(turn), stop)
            left = jnp.where(taken, 0.0, left)
            rows_table[pl.ds(step * 8 + turn, 1), :] = best
            if turn + 1 in UNITS:
                trouble = jnp.maximum(trouble, left * (UNITS.index(turn + 1) + 1.0))
        stops[step] = stop
    codes = rows_table[...]
    codes = jnp.maximum(codes - 128 * jnp.floor(codes / 128) - 1.0, 0.0)
    table[:, : codes.shape[0]] = codes.T
    across[:, :depth] = jnp.where(crosses, order + 1.0, 0.0).T
    ahead[:, :depth] = stops[jnp.maximum(place - 1, 0)].T
    behind[:, :depth] = stops[jnp.maximum(length - 2 - place, 0)].T

    here, there = (lane * 2) * col_size + col, (lane * 2 + 1) * col_size + col
    other = (1 - lane) * 2 * col_size + col
    tile, tile_number = iota((1, lanes), 1), lax.rem(iota((1, lanes), 1), slots)
    tile_place = tile_home // 2
    my_rows, my_cols = tile_row[pl.ds(col, 1), :], tile_col[pl.ds(col, 1), :]
    beyond, under = ahead[pl.ds(here, 1), :], behind[pl.ds(there, 1), :]
    spot = jnp.where(tile_place < place, 2 * slots + beyond, 2 * slots + ROOM + under)
    spot = jnp.where(tile_place == place, slots - 1 + across[pl.ds(here, 1), :], spot)
    spot = jnp.where(tile_home == row, tile_number.astype(F32), spot)

    inside = iota((blocks, blocks), 0), iota((blocks, blocks), 1)
    same_rows = inside[0] // block_rows == inside[1] // block_rows
    same_cols = inside[0] // block_cols == inside[1] // block_cols
    lower = (same_rows & (inside[1] < inside[0])).astype(F32).astype(BF16)
    whole = same_cols.astype(F32).astype(BF16)
    upper = (same_cols & (inside[0] < inside[1])).astype(F32).astype(BF16)
    chip_of = inside[1] // (2 * block_cols)
    flipped = occupied.T.astype(BF16)
    shared = dot(grid, flipped)
    inner = near_count = jnp.zeros((blocks, blocks), F32)
    for chip in range(col_size // 2):
        on_chip = jnp.where(chip_of == chip, occupied, 0.0).astype(BF16)
        inner = jnp.where(chip_of == chip, dot(on_chip, flipped), inner)
        near_count = jnp.where(chip_of == chip, dot(on_chip, grid), near_count)
    leaves = jnp.where((occupied > 0) & (shared > inner), 1.0, 0.0)
    gone = leaves.astype(BF16)
    ranks = dot(dot(lower, grid).astype(BF16), whole) + dot(grid, upper)
    y_ranks = dot(dot(lower, gone).astype(BF16), whole) + dot(gone, upper)
    panels = ((inside[1] // block_cols) * slots).astype(F32)
    labels = ranks + panels
    y_labels = jnp.where(chip_of == col // 2, ranks, y_ranks) + panels
    y_order = leaves * (y_ranks + 1.0)

    def peak(value):
        return jnp.max(jnp.max(value, axis=1, keepdims=True), axis=0, keepdims=True)

    joint = dot(grid, grid)
    fan = peak(joint * occupied)
    crowd = jnp.maximum(peak(y_order) - Y_SLOTS, peak((joint - near_count) * occupied) - FAR_TERMS)

    chosen = (at == my_rows).astype(F32).astype(BF16)
    met = dot(grid, chosen)
    named, y_named = dot(labels.astype(BF16), chosen), dot(y_labels.astype(BF16), chosen)
    sub, column = iota((8, lanes), 0), iota((8, lanes), 1)
    deep, wide = iota((16, lanes), 0), iota((16, lanes), 1)
    pairs = jnp.zeros((16, lanes), F32)
    near = jnp.floor((my_rows + 0.5) / (2 * block_cols)) == (col // 2).astype(F32)
    result = jnp.where(sub == 0, table[pl.ds(here, 1), :], 0.0)
    result = jnp.where(sub == 1, table[pl.ds(there, 1), :], result)
    inside_rows, inside_cols = inside[0].astype(F32), inside[1].astype(F32)
    for slot in range(slots):
        mine = tile == row * slots + slot
        out_row = jnp.sum(jnp.where(mine, my_rows, 0.0), axis=1, keepdims=True)
        out_col = jnp.sum(jnp.where(mine, my_cols, 0.0), axis=1, keepdims=True)
        on_row = at == out_row
        joins = jnp.sum(jnp.where(on_row, met, 0.0), axis=0, keepdims=True)
        name = jnp.sum(jnp.where(on_row, named, 0.0), axis=0, keepdims=True)
        y_name = jnp.sum(jnp.where(on_row, y_named, 0.0), axis=0, keepdims=True)
        use = (joins > 0) & (my_cols == out_col) & (my_rows >= 0)
        pairs = jnp.where((deep == slot) & use, name * 64 + spot + 1, pairs)
        pairs = jnp.where((deep == slot + slots) & use & near, y_name * 64 + spot + 1, pairs)
        pairs = jnp.where((deep == slot + 2 * slots) & use & jnp.logical_not(near), y_name * 64 + spot + 1, pairs)
        y_spot = jnp.where((inside_rows == out_row) & (inside_cols == out_col), y_order, 0.0)
        y_spot = jnp.sum(jnp.sum(y_spot, axis=1, keepdims=True), axis=0, keepdims=True)
        result = jnp.where((sub == 6) & (column == 8 + slot), y_spot, result)
    product = jnp.zeros((16, lanes), F32)
    shifted = wide - 16 * (deep // slots)
    for term in range(TERMS):
        best = jnp.max(pairs, axis=1, keepdims=True)
        pairs = jnp.where(pairs == best, 0.0, pairs)
        product = jnp.where(shifted == term, best, product)

    fetches[1].wait()
    level = peak(trouble)
    kind = 2.0 * level + jnp.where((crowd > 0) & (level < 2), 1.0, 0.0)
    choice[...] = jnp.where(fan > TERMS, 4.0, kind).astype(jnp.int32)
    for slot in range(slots):
        mine = tile == row * slots + slot
        label = ids[0:1, slot : slot + 1].astype(F32)
        owner = (tile_home == row) & (tile_spot[pl.ds(col, 1), :] == label)
        name = jnp.sum(jnp.where(owner, tile_number.astype(F32) + 1.0, 0.0), axis=1, keepdims=True)
        order = jnp.where(mine, across[pl.ds(other, 1), :], 0.0)
        order = jnp.sum(order, axis=1, keepdims=True)
        result = jnp.where((sub == 6) & (column == slot), name, result)
        result = jnp.where((sub == 2) & (column == slot), order, result)
        every = jnp.where(lax.rem(deep, slots) == slot, product, 0.0)
        result = jnp.where(sub == 3 + slot, jnp.sum(every, axis=0, keepdims=True), result)
    out[...] = result.astype(jnp.int32)
    fetches[2].wait()


def make_plan(mesh, mask, ids, stack):
    row_size, col_size = mesh.shape["row"], mesh.shape["col"]
    slots, steps = stack.shape[0], row_size // 2 - 1
    panel, lines = pltpu.VMEM((col_size, 128), F32), 4 * col_size
    wide = pltpu.VMEM((lines, 128), F32)
    return pl.pallas_call(
        functools.partial(plan_kernel, row_size, col_size, slots),
        out_shape=(
            jax.ShapeDtypeStruct((8, 128), jnp.int32),
            jax.ShapeDtypeStruct((1, 1), jnp.int32),
            jax.ShapeDtypeStruct(stack.shape, stack.dtype),
        ),
        in_specs=[HBM, HBM, HBM],
        out_specs=(VMEM, VMEM, VMEM),
        scratch_shapes=[
            pltpu.VMEM(mask.shape, mask.dtype), pltpu.VMEM(ids.shape, ids.dtype), panel, panel, panel, wide, wide,
            pltpu.VMEM((8 * steps, lines), F32), wide, wide, wide, wide,
            pltpu.VMEM((steps, row_size * slots, lines), F32), pltpu.SemaphoreType.DMA((3,)),
        ],
        compiler_params=pltpu.CompilerParams(vmem_limit_bytes=16 * 2**20),
        name="plan",
    )(mask, ids, stack)


def sparse_kernel(
    row_size, col_size, units, y_slots, far_terms, table, tiles, out, canon, x_out, left, held, squares, near, square,
    total, final, y_out, z_out, plan, col_sems, square_sems, x_sems, z_sems, plan_sem,
):
    row, col = lax.axis_index("row"), lax.axis_index("col")
    slots, side = canon.shape[0], canon.shape[1]
    rows = side // PARTS
    length = row_size // 2
    place, lane = row // 2, lax.rem(row, 2)
    mate = row + 1 - 2 * lane
    chips = col_size // 2
    chip, core = col // 2, lax.rem(col, 2)
    x_units = slots

    barrier = pltpu.get_barrier_semaphore()

    def hello(to_row, to_col):
        pl.semaphore_signal(barrier, inc=1, device_id=(to_row, to_col), device_id_type=MESH)

    fetch = pltpu.make_async_copy(table, plan, plan_sem)
    fetch.start()
    hello(mate, col)
    hello(row, col + 1 - 2 * core)
    for step in range(1, chips):
        hello(row, 2 * lax.rem(chip + step, chips) + core)
    for way in range(2):
        @pl.when((place + 1 < length) if way == 0 else (place > 0))
        def _():
            hello(row + 2 - 4 * way, col)

    fetch.wait()
    for number in range(slots):
        tile = jnp.zeros((side, side), tiles.dtype)
        for slot in range(slots):
            tile = jnp.where(plan[6, slot] == number + 1, tiles[slot], tile)
        canon[number] = tile
    for slot in range(slots):
        tile = canon[0]
        for number in range(1, slots):
            tile = jnp.where(plan[2, number] == slot + 1, canon[number], tile)
        x_out[slot] = tile

    ends = jnp.where(place == 0, 1, 0) + jnp.where(place + 1 == length, 1, 0)
    pl.semaphore_wait(barrier, 2 + chips - 1 + 2 - ends)

    def x_copy(unit, part):
        span = pl.ds(part * rows, rows)
        return send(
            x_out.at[unit, span], held.at[slots + unit, span],
            x_sems.at[0, unit, part], x_sems.at[1, unit, part], mate, col,
        )

    def z_copy(way, unit, part):
        span = pl.ds(part * rows, rows)
        return send(
            z_out.at[way, unit, span], held.at[2 * slots + way * ROOM + unit, span],
            z_sems.at[way, 0, unit, part], z_sems.at[way, 1, unit, part], row + 2 - 4 * way, col,
        )

    for unit in range(x_units):
        for part in range(PARTS):
            x_copy(unit, part).start()
    left_gather = ColGather(row, col, col_size, slots, canon, left, col_sems)
    left_gather.start()

    done = (place, length - 1 - place)
    for unit in range(units):
        for way in range(2):
            @pl.when(done[way] + 1 < length)
            def _():
                code = plan[way, done[way] * 8 + unit]
                piece = canon[0]
                for other in range(1, slots):
                    piece = jnp.where(code == other, canon[other], piece)
                for other in range(min(unit - 1, x_units)):
                    piece = jnp.where(code == slots + other, held[slots + other], piece)
                for other in range(unit - 1):
                    piece = jnp.where(code == 2 * slots + other, held[2 * slots + way * ROOM + other], piece)
                z_out[way, unit] = piece

        for part in range(PARTS):
            span = pl.ds(part * rows, rows)
            if 1 <= unit <= x_units:
                x_copy(unit - 1, part).wait_recv()
            for way in range(2):
                @pl.when(done[way] + 1 < length)
                def _():
                    if unit:
                        @pl.when(done[way] > 0)
                        def _():
                            z_copy(way, unit - 1, part).wait_recv()

                        code = plan[way, done[way] * 8 + unit]
                        piece = z_out[way, unit, span]
                        if unit <= x_units:
                            spot = slots + unit - 1
                            piece = jnp.where(code == spot, held[spot, span], piece)
                        spot = 2 * slots + unit - 1
                        piece = jnp.where(code == spot, held[spot + way * ROOM, span], piece)
                        z_out[way, unit, span] = piece
                    z_copy(way, unit, part).start()

    left_gather.forward()
    for number in range(slots):
        held[number] = canon[number]
        left[col, number] = canon[number]

    for unit in range(units - 1, x_units):
        for part in range(PARTS):
            x_copy(unit, part).wait_recv()
    for way in range(2):
        @pl.when(done[way] + 1 == length)
        def _():
            for unit in range(units - 1):
                for part in range(PARTS):
                    z_copy(way, unit, part).wait_recv()

        @pl.when(done[way] > 0)
        def _():
            for part in range(PARTS):
                z_copy(way, units - 1, part).wait_recv()

    left_gather.collect(None, range(left_gather.chips))

    def sum_terms(panel, number, first, terms):
        result = jnp.zeros((side, side), F32)
        for term in range(terms):
            code = plan[3 + number, first + term]
            pair = jnp.maximum(code - 1, 0)
            name, spot = pair // 64, lax.rem(pair, 64)
            tile = panel[lax.rem(name // slots, panel.shape[0]), lax.rem(name, slots)]
            result += jnp.dot(
                jnp.where(code > 0, tile, jnp.zeros_like(tile)), held[spot], preferred_element_type=F32,
            )
        return result

    square_gather = ColGather(row, col, col_size, slots, square, squares, square_sems, y_out, y_slots, near)

    for slot in range(y_slots):
        number = jnp.int32(0)
        for other in range(1, slots):
            number = jnp.where(plan[6, 8 + other] == slot + 1, other, number)
        y_out[slot] = sum_terms(left, number, 0, TERMS).astype(square.dtype)
        for step in range(1, chips):
            square_gather.across(step, slot).start()

    def first(number, unused):
        tile = sum_terms(left, number, 0, TERMS).astype(square.dtype)
        square[number] = tile
        near[core, number] = tile
        square_gather.beside(0, number).start()
        return unused

    lax.fori_loop(0, slots, first, 0)
    square_gather.collect(None, [0])

    def second(number, unused):
        total[number] = sum_terms(near, number, 16, TERMS)
        return unused

    lax.fori_loop(0, slots, second, 0)
    square_gather.forward()
    square_gather.collect(None, range(1, chips))

    def third(number, unused):
        cube = total[number] + sum_terms(squares, number, 32, far_terms)
        final[number] = (3.0 * square[number].astype(F32) - 2.0 * cube).astype(final.dtype)
        return unused

    lax.fori_loop(0, slots, third, 0)
    for slot in range(slots):
        tile = jnp.zeros((side, side), out.dtype)
        for number in range(slots):
            tile = jnp.where(plan[6, slot] == number + 1, final[number], tile)
        out[slot] = tile

    left_gather.settle()
    square_gather.settle()

    for part in range(PARTS):
        for unit in range(x_units):
            x_copy(unit, part).wait_send()
    for way in range(2):
        @pl.when(done[way] + 1 < length)
        def _():
            for unit in range(units):
                for part in range(PARTS):
                    z_copy(way, unit, part).wait_send()


def room(panels, slots, side):
    return (4 * panels + 16) * slots * side * side * 2 + 8 * 2**20


def sparse_step(mesh, units, y_slots, far_terms, barrier_id, plan, stack):
    row_size, col_size = mesh.shape["row"], mesh.shape["col"]
    chips = col_size // 2
    slots, side, _ = stack.shape
    dma = pltpu.SemaphoreType.DMA

    def tiles(*count):
        return pltpu.VMEM((*count, side, side), stack.dtype)

    return pl.pallas_call(
        functools.partial(sparse_kernel, row_size, col_size, units, y_slots, far_terms),
        out_shape=jax.ShapeDtypeStruct(stack.shape, stack.dtype),
        in_specs=[VMEM, VMEM],
        out_specs=VMEM,
        scratch_shapes=[
            tiles(slots), tiles(slots), tiles(col_size, slots), tiles(2 * slots + 2 * ROOM), tiles(col_size, slots),
            tiles(2, slots), tiles(slots), pltpu.VMEM(stack.shape, F32), tiles(slots), tiles(y_slots), tiles(2, units), pltpu.SMEM(plan.shape, plan.dtype),
            dma((4, chips, slots)), dma((4, chips, slots)), dma((2, slots, PARTS)), dma((2, 2, units, PARTS)), dma,
        ],
        compiler_params=pltpu.CompilerParams(
            collective_id=barrier_id, has_side_effects=True, vmem_limit_bytes=room(col_size, slots, side)
        ),
        name="sparse",
    )(plan, stack)


def dense_step(mesh, ids, stack, mask):
    row_size, col_size = mesh.shape["row"], mesh.shape["col"]
    length, chips = row_size // 2, col_size // 2
    dma = pltpu.SemaphoreType.DMA
    slots, side, _ = stack.shape
    col_panel = pltpu.VMEM((col_size, slots, side, side), stack.dtype)
    return pl.pallas_call(
        functools.partial(dense_kernel, row_size, col_size),
        out_shape=jax.ShapeDtypeStruct(stack.shape, stack.dtype),
        in_specs=[VMEM, SMEM, SMEM],
        out_specs=VMEM,
        scratch_shapes=[
            col_panel,
            pltpu.VMEM((row_size, slots, side, side), stack.dtype),
            col_panel,
            pltpu.VMEM(stack.shape, stack.dtype),
            pltpu.VMEM(stack.shape, jnp.float32),
            pltpu.VMEM((col_size, 8, 128), jnp.int32),
            pltpu.VMEM((row_size, 8, 128), jnp.int32),
            pltpu.VMEM((8, 128), jnp.int32),
            pltpu.SMEM((col_size, 8, 128), jnp.int32),
            pltpu.SMEM((row_size, 8, 128), jnp.int32),
            dma((4, chips, slots)),
            dma((4, chips, slots)),
            dma((2, 2, length, slots + 2)),
            dma((2, length, slots + 1)),
            dma((2, row_size)),
            dma((2, col_size)),
            dma((2,)),
        ],
        compiler_params=pltpu.CompilerParams(
            collective_id=0, has_side_effects=True, vmem_limit_bytes=room(row_size + col_size, slots, side)
        ),
        name="purify",
    )(stack, ids, mask)


def solution(mesh):
    def local(tiles, stack_index, block_mask):
        stack = tiles[0, 0]
        plan, choice, fetched = make_plan(mesh, block_mask, stack_index[0], stack)
        slots = stack.shape[0]
        sizes = (
            (UNITS[0], Y_SLOTS, FAR_TERMS), (UNITS[0], slots, TERMS),
            (UNITS[1], Y_SLOTS, FAR_TERMS), (UNITS[1], slots, TERMS),
        )
        branches = [
            functools.partial(sparse_step, mesh, *size, number + 1, plan, fetched) for number, size in enumerate(sizes)
        ]
        branches = [lambda branch=branch: branch() for branch in branches]
        branches.append(lambda: dense_step(mesh, stack_index[0], stack, block_mask))
        purified = _switch_internal(choice[0, 0], branches, (), branches_platforms=None)
        return purified[None, None]

    placed = (P("row", "col", None, None, None), P("row", "col", None), P())
    return jax.shard_map(
        local,
        mesh=mesh,
        in_specs=placed,
        out_specs=P("row", "col", None, None, None),
        check_vma=False,
    )
```

```python
import functools

import jax
import jax.numpy as jnp
from jax import lax
from jax.experimental import pallas as pl
from jax.experimental.pallas import tpu as pltpu
from jax.sharding import PartitionSpec as P
from jax._src.lax.control_flow.conditionals import _switch_internal

MESH = pl.DeviceIdType.MESH
VMEM = pl.BlockSpec(memory_space=pltpu.VMEM)
SMEM = pl.BlockSpec(memory_space=pltpu.SMEM)
HBM = pl.BlockSpec(memory_space=pltpu.HBM)


def send(src, dst, send_sem, recv_sem, row, col):
    return pltpu.make_async_remote_copy(
        src_ref=src,
        dst_ref=dst,
        send_sem=send_sem,
        recv_sem=recv_sem,
        device_id=(row, col),
        device_id_type=MESH,
    )


def greet(row_size, col_size, row, col, with_rows):
    barrier = pltpu.get_barrier_semaphore()
    count = col_size - 1
    for step in range(1, col_size):
        peer = lax.rem(col + step, col_size)
        pl.semaphore_signal(barrier, inc=1, device_id=(row, peer), device_id_type=MESH)
    if with_rows:
        count += row_size - 1
        for step in range(1, row_size):
            peer = lax.rem(row + step, row_size)
            pl.semaphore_signal(barrier, inc=1, device_id=(peer, col), device_id_type=MESH)
    pl.semaphore_wait(barrier, count)


class ColGather:
    def __init__(self, row, col, col_size, slots, own, panel, sems, far=None, far_slots=None, near=None):
        self.row, self.col, self.slots = row, col, slots
        self.own, self.panel, self.sems = own, panel, sems
        self.far, self.near = own if far is None else far, near
        self.far_slots = slots if far_slots is None else far_slots
        self.chips = col_size // 2
        self.chip, self.core = col // 2, lax.rem(col, 2)
        self.partner = col + 1 - 2 * self.core

    def across(self, step, slot):
        target = 2 * lax.rem(self.chip + step, self.chips) + self.core
        return send(
            self.far.at[slot], self.panel.at[self.col, slot],
            self.sems.at[0, step - 1, slot], self.sems.at[1, step - 1, slot], self.row, target,
        )

    def beside(self, step, slot):
        origin = 2 * lax.rem(self.chip + self.chips - step, self.chips) + self.core
        src = self.own.at[slot] if step == 0 else self.panel.at[origin, slot]
        near = self.near is not None and step == 0
        return send(
            src, self.near.at[self.core, slot] if near else self.panel.at[origin, slot],
            self.sems.at[2, step, slot], self.sems.at[3, step, slot], self.row, self.partner,
        )

    def start(self):
        for slot in range(self.slots):
            for step in range(1, self.chips):
                self.across(step, slot).start()
        for slot in range(self.slots):
            self.beside(0, slot).start()

    def origin(self, step, core):
        return 2 * lax.rem(self.chip + self.chips - step, self.chips) + core

    def forward(self, use=None):
        for slot in range(self.far_slots):
            for step in range(1, self.chips):
                self.across(step, slot).wait_recv()
                self.beside(step, slot).start()
                if use is not None:
                    use(self.origin(step, self.core), slot)

    def count(self, step):
        return self.far_slots if step else self.slots

    def collect(self, use, steps):
        for step in steps:
            for slot in range(self.count(step)):
                self.beside(step, slot).wait_recv()
                if use is not None:
                    use(self.origin(step, 1 - self.core), slot)

    def settle(self):
        for step in range(self.chips):
            for slot in range(self.count(step)):
                if step:
                    self.across(step, slot).wait_send()
                self.beside(step, slot).wait_send()


def dense_kernel(
    row_size, col_size, tiles, ids, mask, out, left, right, squares, square, total, left_ids, right_ids, ids_out,
    left_labels, right_labels, col_sems, square_sems, line_sems, side_sems, row_id_sems, col_id_sems, label_sems,
):
    row, col = lax.axis_index("row"), lax.axis_index("col")
    slots, side = tiles.shape[0], tiles.shape[1]
    half = side // 2
    length = row_size // 2
    place, lane = row // 2, lax.rem(row, 2)
    mate = row + 1 - 2 * lane

    lane_iota = lax.broadcasted_iota(jnp.int32, (8, 128), 1)
    packed = jnp.full((8, 128), -1, jnp.int32)
    for slot in range(slots):
        packed = jnp.where(lane_iota == slot, ids[0, slot], packed)
    ids_out[...] = packed
    greet(row_size, col_size, row, col, True)

    pieces = [(slot, 0, side, False) for slot in range(slots - 1)]
    cut = side * 64 // 256
    pieces += [(slots - 1, cut, side - cut, False)]
    early = (slots - 1, 0, cut, True)
    mine = [early] + pieces
    count = len(mine)

    def view(ref, piece, origin=None):
        slot, first, rows, _ = piece
        if origin is None:
            return ref.at[slot, pl.ds(first, rows)]
        return ref.at[origin, slot, pl.ds(first, rows)]

    def to_mate(index, at):
        piece = mine[index]
        origin = 2 * at + lane
        return send(
            view(right, piece, origin), view(right, piece, origin),
            side_sems.at[0, at, index], side_sems.at[1, at, index], mate, col,
        )

    def own_to_mate(index):
        piece = mine[index]
        return send(
            view(tiles, piece), view(right, piece, row),
            side_sems.at[0, place, index], side_sems.at[1, place, index], mate, col,
        )

    def from_mate(index, at):
        piece = mine[index]
        origin = 2 * at + 1 - lane
        return send(
            view(right, piece, origin), view(right, piece, origin),
            side_sems.at[0, at, index], side_sems.at[1, at, index], mate, col,
        )

    def along(way, step, index, first=False):
        heading = 1 if way == 0 else -1
        piece = mine[0] if index == count else mine[index]
        on_lane = 1 - lane if index == count else lane
        origin = 2 * (place - heading * step) + on_lane
        src = view(tiles, piece) if first and index < count else view(right, piece, origin)
        return send(
            src, view(right, piece, origin),
            line_sems.at[way, 0, step, index], line_sems.at[way, 1, step, index],
            row + 2 * heading, col,
        )

    def landing(way, step, index):
        heading = 1 if way == 0 else -1
        piece = mine[0] if index == count else mine[index]
        on_lane = 1 - lane if index == count else lane
        origin = 2 * (place - heading * (step + 1)) + on_lane
        return send(
            view(right, piece, origin), view(right, piece, origin),
            line_sems.at[way, 0, step, index], line_sems.at[way, 1, step, index],
            row + 2 * heading, col,
        )

    can_send = (place + 1 < length, place > 0)

    def arrives(way, step):
        return place - step >= 1 if way == 0 else place + step + 1 < length

    def goes(way, step):
        if way == 0:
            return (place - step >= 0) & (place + 1 < length)
        return (place + step < length) & (place > 0)

    def id_row(step):
        return send(
            ids_out, right_ids.at[row], row_id_sems.at[0, step], row_id_sems.at[1, step],
            lax.rem(row + step, row_size), col,
        )

    def id_col(step):
        return send(
            ids_out, left_ids.at[col], col_id_sems.at[0, step], col_id_sems.at[1, step],
            row, lax.rem(col + step, col_size),
        )

    for step in range(1, row_size):
        id_row(step).start()
    for step in range(1, col_size):
        id_col(step).start()

    left_gather = ColGather(row, col, col_size, slots, tiles, left, col_sems)
    left_gather.start()
    own_to_mate(0).start()
    for index in range(count):
        for way in range(2):
            @pl.when(can_send[way])
            def _():
                along(way, 0, index, True).start()
        if index:
            own_to_mate(index).start()


    from_mate(0, place).wait_recv()
    for way in range(2):
        @pl.when(can_send[way])
        def _():
            along(way, 0, count).start()

    right[row] = tiles[...]
    left[col] = tiles[...]
    right_ids[row] = packed
    left_ids[col] = packed

    def turn(step, unused):
        for index in list(range(count)) + [count]:
            for way in range(2):
                @pl.when(arrives(way, step))
                def _():
                    landing(way, step, index).wait_recv()

                    @pl.when(can_send[way])
                    def _():
                        along(way, step + 1, index).start()

                    if 0 < index < count:
                        heading = 1 if way == 0 else -1
                        to_mate(index, place - heading * (step + 1)).start()
        return unused

    block_rows, block_cols = mask.shape[0] // row_size, mask.shape[1] // col_size
    owns = []
    for slot in range(slots):
        own = ids[0, slot]
        own_row, own_col = own // block_cols, lax.rem(own, block_cols)
        out_row, out_col = row * block_rows + own_row, col * block_cols + own_col
        owns.append((own_row, own_col, out_row, out_col, mask[out_row, out_col] > 0))

    def find(labels, region, wanted):
        spot, found = jnp.int32(0), labels[region, 0, 0] == wanted
        for other in range(1, slots):
            same = labels[region, 0, other] == wanted
            spot = jnp.where(same, other, spot)
            found = found | same
        return spot, found

    def square_term(origin, place):
        label = right_labels[origin, 0, place]
        inner = origin * block_rows + label // block_cols
        band = inner // block_cols
        chosen = []
        for own_row, own_col, out_row, out_col, live in owns:
            spot, found = find(left_labels, band, own_row * block_cols + lax.rem(inner, block_cols))
            use = live & found & (lax.rem(label, block_cols) == own_col)
            use = use & (mask[out_row, inner] > 0) & (mask[inner, out_col] > 0)
            tile = left[band, spot]
            chosen.append(jnp.where(use, tile, jnp.zeros_like(tile)))
        term = jnp.dot(
            jnp.concatenate(chosen, axis=0), right[origin, place], preferred_element_type=jnp.float32
        )
        total[...] += term.reshape(total.shape)

    def cube_term(origin, place):
        label = left_labels[origin, 0, place]
        inner = origin * block_cols + lax.rem(label, block_cols)
        band = inner // block_rows
        piece = squares[origin, place]
        for slot, (own_row, own_col, out_row, out_col, live) in enumerate(owns):
            spot, found = find(right_labels, band, lax.rem(inner, block_rows) * block_cols + own_col)
            use = live & found & (label // block_cols == own_row)
            use = use & (mask[out_row, inner] > 0) & (mask[inner, out_col] > 0)
            tile = right[band, spot]
            total[slot] += jnp.dot(
                piece, jnp.where(use, tile, jnp.zeros_like(tile)), preferred_element_type=jnp.float32
            )

    def stack_terms(origin, wait=None):
        for slot in range(slots):
            if wait is not None:
                wait(slot)
            square_term(origin, slot)

    def mate_terms(at):
        stack_terms(2 * at + 1 - lane, lambda slot: from_mate(slot + 1, at).wait_recv())

    def consume(step):
        for way in range(2):
            @pl.when(arrives(way, step))
            def _():
                heading = 1 if way == 0 else -1
                stack_terms(2 * (place - heading * (step + 1)) + lane)
        for way in range(2):
            @pl.when(arrives(way, step))
            def _():
                heading = 1 if way == 0 else -1
                mate_terms(place - heading * (step + 1))

    total[...] = jnp.zeros_like(total)
    turn(0, 0)
    for step in range(1, row_size):
        id_row(step).wait()
    for step in range(1, col_size):
        id_col(step).wait()
    copies = (
        pltpu.make_async_copy(left_ids, left_labels, label_sems.at[0]),
        pltpu.make_async_copy(right_ids, right_labels, label_sems.at[1]),
    )
    for copy in copies:
        copy.start()
    for copy in copies:
        copy.wait()
    left_gather.forward()
    left_gather.collect(None, range(left_gather.chips))
    stack_terms(row)
    mate_terms(place)

    def advance(step, unused):
        turn(step, 0)
        consume(step - 1)
        return unused

    lax.fori_loop(1, length - 1, advance, 0)
    consume(length - 2)

    square[...] = total[...].astype(square.dtype)

    square_gather = ColGather(row, col, col_size, slots, square, squares, square_sems)

    def keep(slot, unused):
        squares[col, slot] = square[slot]
        for step in range(1, square_gather.chips):
            square_gather.across(step, slot).start()
        square_gather.beside(0, slot).start()
        return unused

    lax.fori_loop(0, slots, keep, 0)
    total[...] = jnp.zeros_like(total)
    for slot in range(slots):
        cube_term(col, slot)
    square_gather.collect(cube_term, [0])
    square_gather.forward(cube_term)
    square_gather.collect(cube_term, range(1, square_gather.chips))
    out[...] = (3.0 * square[...].astype(jnp.float32) - 2.0 * total[...]).astype(out.dtype)

    left_gather.settle()
    square_gather.settle()

    def settle(step, unused):
        for index in range(count + 1):
            for way in range(2):
                @pl.when(goes(way, step))
                def _():
                    along(way, step, index).wait_send()
        return unused

    lax.fori_loop(0, length - 1, settle, 0)
    own_to_mate(0).wait_send()

    def collect(at, unused):
        for index in range(1, count):
            to_mate(index, at).wait_send()
        return unused

    lax.fori_loop(0, length, collect, 0)

UNITS = (4, 5)
ROOM = 5
Y_SLOTS = 2
FAR_TERMS = 2
TERMS = 4
PARTS = 4
F32, BF16 = jnp.float32, jnp.bfloat16


def iota(shape, axis):
    return lax.broadcasted_iota(jnp.int32, shape, axis)


def plan_kernel(
    row_size, col_size, slots, far_mask, far_ids, far_tiles, out, choice, tiles, mask, ids, tile_row, tile_col,
    tile_spot, reach, ranges, rows_table, table, across, ahead, behind, stops, sems,
):
    fetches = [
        pltpu.make_async_copy(src, dst, sems.at[number])
        for number, (src, dst) in enumerate(((far_mask, mask), (far_ids, ids), (far_tiles, tiles)))
    ]
    for fetch in fetches:
        fetch.start()
    blocks, lanes = mask.shape[0], 128
    block_rows, block_cols = blocks // row_size, blocks // col_size
    length = row_size // 2
    lines = 4 * col_size
    row, col = lax.axis_index("row"), lax.axis_index("col")
    place, lane = row // 2, lax.rem(row, 2)
    dot = functools.partial(jnp.dot, preferred_element_type=F32)

    fetches[0].wait()
    occupied = mask[...].astype(F32)
    grid = occupied.astype(BF16)
    row_of, lane_of = iota((blocks, lanes), 0), iota((blocks, lanes), 1)
    spread = row_of - lax.rem(lane_of, block_cols)
    keep = lax.rem(row_of, block_rows) == lane_of // block_cols
    before = (iota((lanes, lanes), 0) <= iota((lanes, lanes), 1)).astype(F32).astype(BF16)
    region_of, spot_of = iota((row_size, lanes), 0), iota((row_size, lanes), 1)
    home = spot_of // slots
    tile_home = iota((1, lanes), 1) // slots
    at = row_of.astype(F32)

    def groups(value):
        return jnp.sum(value.reshape(row_size, block_rows, lanes), axis=1)

    flat = []
    for panel in range(col_size):
        pick = (spread == panel * block_cols).astype(F32).astype(BF16)
        flat.append(groups(jnp.where(keep, dot(grid, pick), 0.0)))
    flat = jnp.concatenate(flat, axis=0)
    every = iota(flat.shape, 0), iota(flat.shape, 1)
    first_lane, every_value = lax.rem(every[0], row_size) * slots, (every[1] + 1).astype(F32)
    rank = dot(flat.astype(BF16), before)
    spots = jnp.zeros(flat.shape, F32)
    for slot in range(slots):
        found = jnp.where((rank == slot + 1) & (flat > 0), every_value, 0.0)
        found = jnp.sum(found, axis=1, keepdims=True)
        spots = jnp.where(every[1] == first_lane + slot, found, spots)
    spot = jnp.sum(spots.reshape(col_size, row_size, lanes), axis=1) - 1.0
    high = jnp.floor((spot + 0.5) / block_cols)
    base_row = ((iota((col_size, lanes), 1) // slots) * block_rows).astype(F32)
    base_col = (iota((col_size, lanes), 0) * block_cols).astype(F32)
    block_row = jnp.where(spot >= 0, base_row + high, -1.0)
    block_col = jnp.where(spot >= 0, base_col + spot - high * block_cols, -1.0)
    tile_spot[...], tile_row[...], tile_col[...] = spot, block_row, block_col
    by_rows = [
        dot(grid, (at == block_row[panel : panel + 1]).astype(F32).astype(BF16)) for panel in range(col_size)
    ]
    by_cols = [
        dot(grid, (at == block_col[panel : panel + 1]).astype(F32).astype(BF16)) for panel in range(col_size)
    ]
    for panel, (by_row, by_col) in enumerate(zip(by_rows, by_cols)):
        wanted = (groups(by_row * by_col) > 0) & (region_of != home)
        for side in range(2):
            for way in range(2):
                step = region_of // 2 + 1 if way == 0 else length - region_of // 2
                far = jnp.where(wanted & (lax.rem(region_of, 2) == side), step.astype(F32), 0.0)
                reach[pl.ds((side * 2 + way) * col_size + panel, 1), :] = jnp.max(far, axis=0, keepdims=True)
            gap = jnp.abs(region_of // 2 - home // 2) + 1
            gap = jnp.where(wanted & (lax.rem(region_of, 2) == side), gap.astype(F32), 0.0)
            gap = jnp.max(gap, axis=0, keepdims=True)
            for way in range(2):
                ranges[pl.ds((side * 2 + way) * col_size + panel, 1), :] = gap

    depth = row_size * slots
    far, gaps = reach[...].T[:depth], ranges[...].T[:depth]
    tile, line = iota((depth, lines), 0), iota((depth, lines), 1)
    side, way = line // (2 * col_size), lax.rem(line // col_size, 2)
    origin, number = tile // slots, lax.rem(tile, slots)
    begin = jnp.where(way == 0, origin // 2, length - 1 - origin // 2)
    straight = lax.rem(origin, 2) == side
    crosses = (gaps > 0) & jnp.logical_not(straight)
    number_value = number.astype(F32)
    value = jnp.where(crosses, gaps * 8 - number_value, -8.0)
    order = jnp.zeros((depth, lines), F32)
    for back in range(1, slots):
        order += jnp.where((number >= back) & (pltpu.roll(value, back, 0) > value), 1.0, 0.0)
        order += jnp.where((number + back < slots) & (pltpu.roll(value, depth - back, 0) > value), 1.0, 0.0)
    trouble = jnp.zeros((depth, lines), F32)
    first_ready = jnp.where(straight, 0.0, order + 1)
    first_code = jnp.where(straight, number_value, slots + order)
    weight = far * (128 * 128) - (128 * tile).astype(F32) + 1.0
    stop = jnp.zeros((depth, lines), F32)
    for step in range(length - 1):
        fresh = begin == step
        ready = jnp.where(fresh, first_ready, stop + 1.0)
        key = weight + jnp.where(fresh, first_code, 2 * slots + stop)
        left = jnp.where((far > step + 1) & (begin <= step), 1.0, 0.0)
        for turn in range(ROOM):
            live = jnp.where((left > 0) & (ready <= turn), key, 0.0)
            best = jnp.max(live, axis=0, keepdims=True)
            taken = (live == best) & (live > 0)
            stop = jnp.where(taken, float(turn), stop)
            left = jnp.where(taken, 0.0, left)
            rows_table[pl.ds(step * 8 + turn, 1), :] = best
            if turn + 1 in UNITS:
                trouble = jnp.maximum(trouble, left * (UNITS.index(turn + 1) + 1.0))
        stops[step] = stop
    codes = rows_table[...]
    codes = jnp.maximum(codes - 128 * jnp.floor(codes / 128) - 1.0, 0.0)
    table[:, : codes.shape[0]] = codes.T
    across[:, :depth] = jnp.where(crosses, order + 1.0, 0.0).T
    ahead[:, :depth] = stops[jnp.maximum(place - 1, 0)].T
    behind[:, :depth] = stops[jnp.maximum(length - 2 - place, 0)].T

    here, there = (lane * 2) * col_size + col, (lane * 2 + 1) * col_size + col
    other = (1 - lane) * 2 * col_size + col
    tile, tile_number = iota((1, lanes), 1), lax.rem(iota((1, lanes), 1), slots)
    tile_place = tile_home // 2
    my_rows, my_cols = tile_row[pl.ds(col, 1), :], tile_col[pl.ds(col, 1), :]
    beyond, under = ahead[pl.ds(here, 1), :], behind[pl.ds(there, 1), :]
    spot = jnp.where(tile_place < place, 2 * slots + beyond, 2 * slots + ROOM + under)
    spot = jnp.where(tile_place == place, slots - 1 + across[pl.ds(here, 1), :], spot)
    spot = jnp.where(tile_home == row, tile_number.astype(F32), spot)

    inside = iota((blocks, blocks), 0), iota((blocks, blocks), 1)
    same_rows = inside[0] // block_rows == inside[1] // block_rows
    same_cols = inside[0] // block_cols == inside[1] // block_cols
    lower = (same_rows & (inside[1] < inside[0])).astype(F32).astype(BF16)
    whole = same_cols.astype(F32).astype(BF16)
    upper = (same_cols & (inside[0] < inside[1])).astype(F32).astype(BF16)
    chip_of = inside[1] // (2 * block_cols)
    flipped = occupied.T.astype(BF16)
    shared = dot(grid, flipped)
    inner = near_count = jnp.zeros((blocks, blocks), F32)
    for chip in range(col_size // 2):
        on_chip = jnp.where(chip_of == chip, occupied, 0.0).astype(BF16)
        inner = jnp.where(chip_of == chip, dot(on_chip, flipped), inner)
        near_count = jnp.where(chip_of == chip, dot(on_chip, grid), near_count)
    leaves = jnp.where((occupied > 0) & (shared > inner), 1.0, 0.0)
    gone = leaves.astype(BF16)
    ranks = dot(dot(lower, grid).astype(BF16), whole) + dot(grid, upper)
    y_ranks = dot(dot(lower, gone).astype(BF16), whole) + dot(gone, upper)
    panels = ((inside[1] // block_cols) * slots).astype(F32)
    labels = ranks + panels
    y_labels = jnp.where(chip_of == col // 2, ranks, y_ranks) + panels
    y_order = leaves * (y_ranks + 1.0)

    def peak(value):
        return jnp.max(jnp.max(value, axis=1, keepdims=True), axis=0, keepdims=True)

    joint = dot(grid, grid)
    fan = peak(joint * occupied)
    crowd = jnp.maximum(peak(y_order) - Y_SLOTS, peak((joint - near_count) * occupied) - FAR_TERMS)

    chosen = (at == my_rows).astype(F32).astype(BF16)
    met = dot(grid, chosen)
    named, y_named = dot(labels.astype(BF16), chosen), dot(y_labels.astype(BF16), chosen)
    sub, column = iota((8, lanes), 0), iota((8, lanes), 1)
    deep, wide = iota((16, lanes), 0), iota((16, lanes), 1)
    pairs = jnp.zeros((16, lanes), F32)
    near = jnp.floor((my_rows + 0.5) / (2 * block_cols)) == (col // 2).astype(F32)
    result = jnp.where(sub == 0, table[pl.ds(here, 1), :], 0.0)
    result = jnp.where(sub == 1, table[pl.ds(there, 1), :], result)
    inside_rows, inside_cols = inside[0].astype(F32), inside[1].astype(F32)
    for slot in range(slots):
        mine = tile == row * slots + slot
        out_row = jnp.sum(jnp.where(mine, my_rows, 0.0), axis=1, keepdims=True)
        out_col = jnp.sum(jnp.where(mine, my_cols, 0.0), axis=1, keepdims=True)
        on_row = at == out_row
        joins = jnp.sum(jnp.where(on_row, met, 0.0), axis=0, keepdims=True)
        name = jnp.sum(jnp.where(on_row, named, 0.0), axis=0, keepdims=True)
        y_name = jnp.sum(jnp.where(on_row, y_named, 0.0), axis=0, keepdims=True)
        use = (joins > 0) & (my_cols == out_col) & (my_rows >= 0)
        pairs = jnp.where((deep == slot) & use, name * 64 + spot + 1, pairs)
        pairs = jnp.where((deep == slot + slots) & use & near, y_name * 64 + spot + 1, pairs)
        pairs = jnp.where((deep == slot + 2 * slots) & use & jnp.logical_not(near), y_name * 64 + spot + 1, pairs)
        y_spot = jnp.where((inside_rows == out_row) & (inside_cols == out_col), y_order, 0.0)
        y_spot = jnp.sum(jnp.sum(y_spot, axis=1, keepdims=True), axis=0, keepdims=True)
        result = jnp.where((sub == 6) & (column == 8 + slot), y_spot, result)
    product = jnp.zeros((16, lanes), F32)
    shifted = wide - 16 * (deep // slots)
    for term in range(TERMS):
        best = jnp.max(pairs, axis=1, keepdims=True)
        pairs = jnp.where(pairs == best, 0.0, pairs)
        product = jnp.where(shifted == term, best, product)

    fetches[1].wait()
    level = peak(trouble)
    kind = 2.0 * level + jnp.where((crowd > 0) & (level < 2), 1.0, 0.0)
    choice[...] = jnp.where(fan > TERMS, 4.0, kind).astype(jnp.int32)
    for slot in range(slots):
        mine = tile == row * slots + slot
        label = ids[0:1, slot : slot + 1].astype(F32)
        owner = (tile_home == row) & (tile_spot[pl.ds(col, 1), :] == label)
        name = jnp.sum(jnp.where(owner, tile_number.astype(F32) + 1.0, 0.0), axis=1, keepdims=True)
        order = jnp.where(mine, across[pl.ds(other, 1), :], 0.0)
        order = jnp.sum(order, axis=1, keepdims=True)
        result = jnp.where((sub == 6) & (column == slot), name, result)
        result = jnp.where((sub == 2) & (column == slot), order, result)
        every = jnp.where(lax.rem(deep, slots) == slot, product, 0.0)
        result = jnp.where(sub == 3 + slot, jnp.sum(every, axis=0, keepdims=True), result)
    out[...] = result.astype(jnp.int32)
    fetches[2].wait()


def make_plan(mesh, mask, ids, stack):
    row_size, col_size = mesh.shape["row"], mesh.shape["col"]
    slots, steps = stack.shape[0], row_size // 2 - 1
    panel, lines = pltpu.VMEM((col_size, 128), F32), 4 * col_size
    wide = pltpu.VMEM((lines, 128), F32)
    return pl.pallas_call(
        functools.partial(plan_kernel, row_size, col_size, slots),
        out_shape=(
            jax.ShapeDtypeStruct((8, 128), jnp.int32),
            jax.ShapeDtypeStruct((1, 1), jnp.int32),
            jax.ShapeDtypeStruct(stack.shape, stack.dtype),
        ),
        in_specs=[HBM, HBM, HBM],
        out_specs=(VMEM, VMEM, VMEM),
        scratch_shapes=[
            pltpu.VMEM(mask.shape, mask.dtype), pltpu.VMEM(ids.shape, ids.dtype), panel, panel, panel, wide, wide,
            pltpu.VMEM((8 * steps, lines), F32), wide, wide, wide, wide,
            pltpu.VMEM((steps, row_size * slots, lines), F32), pltpu.SemaphoreType.DMA((3,)),
        ],
        compiler_params=pltpu.CompilerParams(vmem_limit_bytes=16 * 2**20),
        name="plan",
    )(mask, ids, stack)


def sparse_kernel(
    row_size, col_size, units, y_slots, far_terms, table, tiles, out, canon, x_out, left, held, squares, near, square,
    total, final, y_out, z_out, plan, col_sems, square_sems, x_sems, z_sems, plan_sem,
):
    row, col = lax.axis_index("row"), lax.axis_index("col")
    slots, side = canon.shape[0], canon.shape[1]
    rows = side // PARTS
    length = row_size // 2
    place, lane = row // 2, lax.rem(row, 2)
    mate = row + 1 - 2 * lane
    chips = col_size // 2
    chip, core = col // 2, lax.rem(col, 2)
    x_units = slots

    barrier = pltpu.get_barrier_semaphore()

    def hello(to_row, to_col):
        pl.semaphore_signal(barrier, inc=1, device_id=(to_row, to_col), device_id_type=MESH)

    fetch = pltpu.make_async_copy(table, plan, plan_sem)
    fetch.start()
    hello(mate, col)
    hello(row, col + 1 - 2 * core)
    for step in range(1, chips):
        hello(row, 2 * lax.rem(chip + step, chips) + core)
    for way in range(2):
        @pl.when((place + 1 < length) if way == 0 else (place > 0))
        def _():
            hello(row + 2 - 4 * way, col)

    fetch.wait()
    for number in range(slots):
        tile = jnp.zeros((side, side), tiles.dtype)
        for slot in range(slots):
            tile = jnp.where(plan[6, slot] == number + 1, tiles[slot], tile)
        canon[number] = tile
    for slot in range(slots):
        tile = canon[0]
        for number in range(1, slots):
            tile = jnp.where(plan[2, number] == slot + 1, canon[number], tile)
        x_out[slot] = tile

    ends = jnp.where(place == 0, 1, 0) + jnp.where(place + 1 == length, 1, 0)
    pl.semaphore_wait(barrier, 2 + chips - 1 + 2 - ends)

    def x_copy(unit, part):
        span = pl.ds(part * rows, rows)
        return send(
            x_out.at[unit, span], held.at[slots + unit, span],
            x_sems.at[0, unit, part], x_sems.at[1, unit, part], mate, col,
        )

    def z_copy(way, unit, part):
        span = pl.ds(part * rows, rows)
        return send(
            z_out.at[way, unit, span], held.at[2 * slots + way * ROOM + unit, span],
            z_sems.at[way, 0, unit, part], z_sems.at[way, 1, unit, part], row + 2 - 4 * way, col,
        )

    for unit in range(x_units):
        for part in range(PARTS):
            x_copy(unit, part).start()
    left_gather = ColGather(row, col, col_size, slots, canon, left, col_sems)
    left_gather.start()

    done = (place, length - 1 - place)
    for unit in range(units):
        for way in range(2):
            @pl.when(done[way] + 1 < length)
            def _():
                code = plan[way, done[way] * 8 + unit]
                piece = canon[0]
                for other in range(1, slots):
                    piece = jnp.where(code == other, canon[other], piece)
                for other in range(min(unit - 1, x_units)):
                    piece = jnp.where(code == slots + other, held[slots + other], piece)
                for other in range(unit - 1):
                    piece = jnp.where(code == 2 * slots + other, held[2 * slots + way * ROOM + other], piece)
                z_out[way, unit] = piece

        for part in range(PARTS):
            span = pl.ds(part * rows, rows)
            if 1 <= unit <= x_units:
                x_copy(unit - 1, part).wait_recv()
            for way in range(2):
                @pl.when(done[way] + 1 < length)
                def _():
                    if unit:
                        @pl.when(done[way] > 0)
                        def _():
                            z_copy(way, unit - 1, part).wait_recv()

                        code = plan[way, done[way] * 8 + unit]
                        piece = z_out[way, unit, span]
                        if unit <= x_units:
                            spot = slots + unit - 1
                            piece = jnp.where(code == spot, held[spot, span], piece)
                        spot = 2 * slots + unit - 1
                        piece = jnp.where(code == spot, held[spot + way * ROOM, span], piece)
                        z_out[way, unit, span] = piece
                    z_copy(way, unit, part).start()

    left_gather.forward()
    for number in range(slots):
        held[number] = canon[number]
        left[col, number] = canon[number]

    for unit in range(units - 1, x_units):
        for part in range(PARTS):
            x_copy(unit, part).wait_recv()
    for way in range(2):
        @pl.when(done[way] + 1 == length)
        def _():
            for unit in range(units - 1):
                for part in range(PARTS):
                    z_copy(way, unit, part).wait_recv()

        @pl.when(done[way] > 0)
        def _():
            for part in range(PARTS):
                z_copy(way, units - 1, part).wait_recv()

    left_gather.collect(None, range(left_gather.chips))

    def sum_terms(panel, number, first, terms):
        result = jnp.zeros((side, side), F32)
        for term in range(terms):
            code = plan[3 + number, first + term]
            pair = jnp.maximum(code - 1, 0)
            name, spot = pair // 64, lax.rem(pair, 64)
            tile = panel[lax.rem(name // slots, panel.shape[0]), lax.rem(name, slots)]
            result += jnp.dot(
                jnp.where(code > 0, tile, jnp.zeros_like(tile)), held[spot], preferred_element_type=F32,
            )
        return result

    square_gather = ColGather(row, col, col_size, slots, square, squares, square_sems, y_out, y_slots, near)

    for slot in range(y_slots):
        number = jnp.int32(0)
        for other in range(1, slots):
            number = jnp.where(plan[6, 8 + other] == slot + 1, other, number)
        y_out[slot] = sum_terms(left, number, 0, TERMS).astype(square.dtype)
        for step in range(1, chips):
            square_gather.across(step, slot).start()

    def first(number, unused):
        tile = sum_terms(left, number, 0, TERMS).astype(square.dtype)
        square[number] = tile
        near[core, number] = tile
        square_gather.beside(0, number).start()
        return unused

    lax.fori_loop(0, slots, first, 0)
    square_gather.collect(None, [0])

    def second(number, unused):
        total[number] = sum_terms(near, number, 16, TERMS)
        return unused

    lax.fori_loop(0, slots, second, 0)
    left_gather.settle()
    for part in range(PARTS):
        for unit in range(x_units):
            x_copy(unit, part).wait_send()
    for way in range(2):
        @pl.when(done[way] + 1 < length)
        def _():
            for unit in range(units):
                for part in range(PARTS):
                    z_copy(way, unit, part).wait_send()

    square_gather.forward()
    square_gather.collect(None, range(1, chips))

    def third(number, unused):
        cube = total[number] + sum_terms(squares, number, 32, far_terms)
        final[number] = (3.0 * square[number].astype(F32) - 2.0 * cube).astype(final.dtype)
        return unused

    lax.fori_loop(0, slots, third, 0)
    for slot in range(slots):
        tile = jnp.zeros((side, side), out.dtype)
        for number in range(slots):
            tile = jnp.where(plan[6, slot] == number + 1, final[number], tile)
        out[slot] = tile

    square_gather.settle()


def room(panels, slots, side):
    return (4 * panels + 16) * slots * side * side * 2 + 8 * 2**20


def sparse_step(mesh, units, y_slots, far_terms, barrier_id, plan, stack):
    row_size, col_size = mesh.shape["row"], mesh.shape["col"]
    chips = col_size // 2
    slots, side, _ = stack.shape
    dma = pltpu.SemaphoreType.DMA

    def tiles(*count):
        return pltpu.VMEM((*count, side, side), stack.dtype)

    return pl.pallas_call(
        functools.partial(sparse_kernel, row_size, col_size, units, y_slots, far_terms),
        out_shape=jax.ShapeDtypeStruct(stack.shape, stack.dtype),
        in_specs=[VMEM, VMEM],
        out_specs=VMEM,
        scratch_shapes=[
            tiles(slots), tiles(slots), tiles(col_size, slots), tiles(2 * slots + 2 * ROOM), tiles(col_size, slots),
            tiles(2, slots), tiles(slots), pltpu.VMEM(stack.shape, F32), tiles(slots), tiles(y_slots), tiles(2, units), pltpu.SMEM(plan.shape, plan.dtype),
            dma((4, chips, slots)), dma((4, chips, slots)), dma((2, slots, PARTS)), dma((2, 2, units, PARTS)), dma,
        ],
        compiler_params=pltpu.CompilerParams(
            collective_id=barrier_id, has_side_effects=True, vmem_limit_bytes=room(col_size, slots, side)
        ),
        name="sparse",
    )(plan, stack)


def dense_step(mesh, ids, stack, mask):
    row_size, col_size = mesh.shape["row"], mesh.shape["col"]
    length, chips = row_size // 2, col_size // 2
    dma = pltpu.SemaphoreType.DMA
    slots, side, _ = stack.shape
    col_panel = pltpu.VMEM((col_size, slots, side, side), stack.dtype)
    return pl.pallas_call(
        functools.partial(dense_kernel, row_size, col_size),
        out_shape=jax.ShapeDtypeStruct(stack.shape, stack.dtype),
        in_specs=[VMEM, SMEM, SMEM],
        out_specs=VMEM,
        scratch_shapes=[
            col_panel,
            pltpu.VMEM((row_size, slots, side, side), stack.dtype),
            col_panel,
            pltpu.VMEM(stack.shape, stack.dtype),
            pltpu.VMEM(stack.shape, jnp.float32),
            pltpu.VMEM((col_size, 8, 128), jnp.int32),
            pltpu.VMEM((row_size, 8, 128), jnp.int32),
            pltpu.VMEM((8, 128), jnp.int32),
            pltpu.SMEM((col_size, 8, 128), jnp.int32),
            pltpu.SMEM((row_size, 8, 128), jnp.int32),
            dma((4, chips, slots)),
            dma((4, chips, slots)),
            dma((2, 2, length, slots + 2)),
            dma((2, length, slots + 1)),
            dma((2, row_size)),
            dma((2, col_size)),
            dma((2,)),
        ],
        compiler_params=pltpu.CompilerParams(
            collective_id=0, has_side_effects=True, vmem_limit_bytes=room(row_size + col_size, slots, side)
        ),
        name="purify",
    )(stack, ids, mask)


def solution(mesh):
    def local(tiles, stack_index, block_mask):
        stack = tiles[0, 0]
        plan, choice, fetched = make_plan(mesh, block_mask, stack_index[0], stack)
        slots = stack.shape[0]
        sizes = (
            (UNITS[0], Y_SLOTS, FAR_TERMS), (UNITS[0], slots, TERMS),
            (UNITS[1], Y_SLOTS, FAR_TERMS), (UNITS[1], slots, TERMS),
        )
        branches = [
            functools.partial(sparse_step, mesh, *size, number + 1, plan, fetched) for number, size in enumerate(sizes)
        ]
        branches = [lambda branch=branch: branch() for branch in branches]
        branches.append(lambda: dense_step(mesh, stack_index[0], stack, block_mask))
        purified = _switch_internal(choice[0, 0], branches, (), branches_platforms=None)
        return purified[None, None]

    placed = (P("row", "col", None, None, None), P("row", "col", None), P())
    return jax.shard_map(
        local,
        mesh=mesh,
        in_specs=placed,
        out_specs=P("row", "col", None, None, None),
        check_vma=False,
    )
```
